256 devices in a mesh: gx: 16 (over z, x_lo), gy: 16 (over y, x_hi, core).
Axes of the slice: x: 4 (x_hi: 2, x_lo: 2; x = x_hi * 2 + x_lo), y: 4, z: 8, core: 2. Of those that a mesh axis runs over, the one named last changes fastest.
Arguments:
- pooled: bfloat16 [32768, 8, 128], P(('gx', 'gy')), may hold values from -6 to 6
- cotangent: bfloat16 [32768, 28, 128], P(('gx', 'gy')), may hold values from -0.03125 to 0.03125
- bilinear: bfloat16 [7, 128, 128], replicated, may hold values from -0.5 to 0.5
- bag_ids: int32 [32768, 8, 4], P(('gx', 'gy')), may hold values from 0 to 65535, as said below
- bag_lens: int32 [32768, 8], P(('gx', 'gy')), may hold values from 1 to 4
- row_home: int32 [8, 65536], replicated, may hold values from 0 to 65535, as said below
Outputs:
- weight_grad: float32 [7, 128, 128], replicated
- table_grad: float32 [65536, 8, 128], P(('gx', 'gy'))
The draws below stay inside these ranges and needn't reach their ends.
Inputs may be any that keep to these rules, and one draw needn't show every extreme that they name: Each row row_home[f] is a permutation; row r of field f's table is stored at position row_home[f, r] of table_grad's first dimension. Only the first bag_lens entries of a bag are live. The stored position q = row_home[f, bag_ids[sample, f, k]] of an entry lies in the block of 256 positions of device q // 256 (devices in gx+gy order); among all entries of one device's samples, live or not, at most 32 lie in any one device's block; in every device's entries some block is hit exactly 32 times, and one block is hit exactly 32 times by the entries of every device.
All inputs are finite; a program needn't handle non-finite values.
Results may differ from the reference program's by a relative error of at most 0.0035.
Values may be sent and summed in bfloat16 or wider, within the bound.
A program may use at most 64 MiB of HBM per device.

```python
import jax
import jax.numpy as jnp
from jax import lax

D = 128
FIELDS = 8
PAIRS = 28
BAG = 4
TOK_DEV = 128
R_DEV = 256
TOKENS = 32768
ROWS = 65536
CAP = 32
N_GX = 16
N_GY = 16


def home_table(key):
    field_keys = jax.random.split(jax.random.fold_in(key, 101), FIELDS)
    return jax.vmap(lambda k: jax.random.permutation(k, ROWS))(field_keys).astype(jnp.int32)


def draw_row_home(key, part):
    return home_table(key)


def draw_bag_ids(key, part):
    home = home_table(key)
    inverse = jnp.argsort(home, axis=1, stable=True).astype(jnp.int32)
    owners_all = N_GX * N_GY
    slots = CAP * owners_all
    entries = TOK_DEV * FIELDS * BAG
    route_key = jax.random.fold_in(key, 202)
    hotness = jax.random.randint(jax.random.fold_in(route_key, 1), (owners_all,), 0, 4).astype(jnp.int32)
    shared_full = jax.random.randint(jax.random.fold_in(route_key, 2), (), 0, owners_all).astype(jnp.int32)
    slot_owner = (jnp.arange(slots, dtype=jnp.int32) // CAP).astype(jnp.int32)

    def one_block(block):
        block_key = jax.random.fold_in(route_key, 1000 + block)
        raw = jax.random.randint(jax.random.fold_in(block_key, 1), (slots,), 0, 4096).astype(jnp.int32)
        score = jnp.right_shift(raw, 2 * hotness[slot_owner])
        own_full = jax.random.randint(jax.random.fold_in(block_key, 2), (), 0, owners_all).astype(jnp.int32)
        forced = jnp.logical_or(slot_owner == own_full, slot_owner == shared_full)
        score = jnp.where(forced, -1, score)
        rank_key = score * slots + jnp.arange(slots, dtype=jnp.int32)
        picked = jnp.argsort(rank_key, stable=True)[:entries]
        owners = slot_owner[picked]
        owners = owners[jax.random.permutation(jax.random.fold_in(block_key, 3), entries)]
        first = jax.random.randint(jax.random.fold_in(block_key, 4), (entries,), 0, R_DEV).astype(jnp.int32)
        second = jax.random.randint(jax.random.fold_in(block_key, 5), (entries,), 0, R_DEV).astype(jnp.int32)
        local = first * second // R_DEV
        return (owners * R_DEV + local).astype(jnp.int32)
    stored = lax.map(one_block, jnp.arange(owners_all, dtype=jnp.int32)).reshape(TOKENS, FIELDS, BAG)
    field_index = jnp.arange(FIELDS, dtype=jnp.int32)[None, :, None]
    return inverse[field_index, stored].astype(jnp.int32)


def plant(result, key, low, high):
    spot = [jax.random.randint(jax.random.fold_in(key, axis), (), 0, length) for axis, length in enumerate(result.shape)]
    widest = result.shape.index(max(result.shape))
    beside = spot[:widest] + [(spot[widest] + 1) % result.shape[widest]] + spot[widest + 1:]
    return result.at[tuple(spot)].set(low).at[tuple(beside)].set(high)


def steps_of(stream_key, extent, cuts, smallest, largest):
    gain = 1.0
    for axis_at, blocks in cuts:
        draws = jax.random.uniform(jax.random.fold_in(jax.random.fold_in(stream_key, 6), axis_at), (blocks,), jnp.float32, smallest / len(cuts), largest / len(cuts))
        gain = gain * jnp.repeat(jnp.exp(draws), extent[axis_at] // blocks).reshape((-1,) + (1,) * (len(extent) - 1 - axis_at))
    return gain


def scatter_about(key, shape, width, most, shards=(), held_as=jnp.bfloat16):
    level = steps_of(key, shape, shards, -0.22, 0.18) if shards else 1.0
    result = jax.random.normal(key, shape, jnp.float32) * width * level
    return jnp.minimum(jnp.maximum(result, -most), most).astype(held_as)


def setup_inputs(seed: int = 0) -> dict:
    key_of = jax.random.split(jax.random.key(seed), 7)
    return {
        "pooled": scatter_about(key_of[0], (TOKENS, FIELDS, D), 1.0, 6.0, ((0, 256),)),
        "cotangent": scatter_about(key_of[1], (TOKENS, PAIRS, D), TOKENS ** -0.5, 0.03125, ((0, 256),)),
        "bilinear": scatter_about(key_of[2], (FIELDS - 1, D, D), D ** -0.5, 0.5),
        "bag_ids": draw_bag_ids(jax.random.fold_in(key_of[6], 71), 0),
        "bag_lens": plant(jax.random.randint(key_of[4], (TOKENS, FIELDS), 1, BAG + 1), jax.random.fold_in(key_of[4], 1), 1, BAG).astype(jnp.int32),
        "row_home": draw_row_home(jax.random.fold_in(key_of[6], 71), 0),
    }


def pair_list(fields):
    return [(i, j) for i in range(fields) for j in range(i + 1, fields)]


def reference(pooled, cotangent, bilinear, bag_ids, bag_lens, row_home):
    pair_order = pair_list(FIELDS)
    embedded = pooled.astype(jnp.float32)
    weights = bilinear.astype(jnp.float32)
    cot_rows = cotangent.astype(jnp.float32)
    projected = jnp.einsum('bfd,fde->bfe', embedded[:, :FIELDS - 1], weights)
    upper_terms = []
    for i in range(FIELDS - 1):
        running = jnp.zeros((TOKENS, D), jnp.float32)
        for p, (a, c) in enumerate(pair_order):
            if a == i:
                running = running + cot_rows[:, p] * embedded[:, c]
        upper_terms.append(running)
    upper_bf = jnp.stack(upper_terms, 1).astype(jnp.bfloat16).astype(jnp.float32)
    weight_grad = jnp.einsum('bfd,bfe->fde', embedded[:, :FIELDS - 1], upper_bf)
    field_list = []
    for i in range(FIELDS):
        running = jnp.zeros((TOKENS, D), jnp.float32)
        if i < FIELDS - 1:
            running = running + jnp.einsum('be,de->bd', upper_bf[:, i], weights[i])
        for p, (a, c) in enumerate(pair_order):
            if c == i:
                running = running + cot_rows[:, p] * projected[:, a]
        field_list.append(running)
    field_grads = jnp.stack(field_list, 1).astype(jnp.bfloat16).astype(jnp.float32)
    live = jnp.arange(BAG, dtype=jnp.int32)[None, :]
    tables = []
    for f in range(FIELDS):
        stored = row_home[f][bag_ids[:, f, :]]
        segment = jnp.where(live < bag_lens[:, f, None], stored, ROWS).astype(jnp.int32)
        values = jnp.broadcast_to(field_grads[:, f, None, :], (TOKENS, BAG, D)).reshape(TOKENS * BAG, D)
        summed = jax.ops.segment_sum(values, segment.reshape(-1), num_segments=ROWS + 1)
        tables.append(summed[:ROWS])
    return weight_grad, jnp.stack(tables, 1)
```

```python
import functools

import jax
import jax.numpy as jnp
from jax import lax
from jax.experimental import pallas as pl
from jax.experimental.pallas import tpu as pltpu
from jax.sharding import PartitionSpec as P

MESH = pl.DeviceIdType.MESH
F = 8
BAG = 4
D = 128
TOK = 128
CAP = 32
NZ = 8
NP = 32
ROWS = F * TOK
NCH = 2
RED = 28
PAIR = {(i, j): p for p, (i, j) in enumerate((i, j) for i in range(F) for j in range(i + 1, F))}
F32, BF16, I32 = jnp.float32, jnp.bfloat16, jnp.int32


def dev(z, p):
    return (2 * z + p // 16, p % 16)


def iota(shape, dim):
    return lax.broadcasted_iota(I32, shape, dim)


def onehot(mask):
    return jnp.where(mask, 1.0, 0.0).astype(BF16)


def dot(a, b, ca=1, cb=0):
    return lax.dot_general(a, b, (((ca,), (cb,)), ((), ())), preferred_element_type=F32)


def body(
    pool_h, cot_h, bil_h, ids_h, lens_h, home_h,
    wg_o, acc_o,
    pool, cot, bil, ids, lens, home,
    pf, up, proj, back, share,
    own, loc, live, m4, mall, dsend, drecv, cbuf,
    vbuf, stage, got, amat, bmat,
    w2, w3, w4, part,
    lsem, zs, zr, ms, mr, ds_, dr, ss, rr, ws, wr,
):
    gx, gy = lax.axis_index("gx"), lax.axis_index("gy")
    z, me = gx // 2, (gx % 2) * 16 + gy
    up_z, dn_z = (z + 1) % NZ, (z + 7) % NZ

    loads = [
        pltpu.make_async_copy(a, b, lsem.at[n])
        for n, (a, b) in enumerate(
            [(pool_h, pool), (bil_h, bil), (cot_h, cot), (ids_h, ids), (lens_h, lens), (home_h, home)]
        )
    ]
    for c in loads:
        c.start()

    bar = pltpu.get_barrier_semaphore()

    @pl.loop(1, NP)
    def _(j):
        pl.semaphore_signal(bar, inc=1, device_id=dev(z, me ^ j), device_id_type=MESH)

    @pl.loop(1, NZ)
    def _(t):
        pl.semaphore_signal(bar, inc=1, device_id=dev((z + t) % NZ, me), device_id_type=MESH)

    loads[0].wait()
    perm = onehot(iota((128, 128), 1) == (iota((128, 128), 0) % 16) * F + iota((128, 128), 0) // 16)
    x = jnp.concatenate([pool[pl.ds(g * 128, 128), :] for g in range(8)], axis=1)
    y = dot(perm, x).astype(BF16)
    for g in range(8):
        for f in range(F):
            pf[f, pl.ds(g * 16, 16), :] = y[f * 16 : f * 16 + 16, g * 128 : g * 128 + 128]
    loads[1].wait()
    for i in range(F - 1):
        proj[i] = dot(pf[i], bil[i])
    loads[2].wait()

    @pl.loop(0, 8)
    def _(r):
        rows = pl.ds(pl.multiple_of(r * 16, 16), 16)
        pj = [pf[j, rows, :].astype(F32) for j in range(F)]
        for i in range(F - 1):
            run = cot[PAIR[i, i + 1], rows, :].astype(F32) * pj[i + 1]
            for j in range(i + 2, F):
                run = run + cot[PAIR[i, j], rows, :].astype(F32) * pj[j]
            up[i, rows, :] = run.astype(BF16)

    for i in range(F - 1):
        back[i] = dot(up[i], bil[i], 1, 1)
    for i in range(F - 1):
        share[pl.ds(i * 128, 128), :] = dot(pf[i], up[i], 0, 0).astype(BF16)

    @pl.loop(0, 8)
    def _(r):
        rows = pl.ds(pl.multiple_of(r * 16, 16), 16)
        for i in range(F):
            run = back[i, rows, :] if i < F - 1 else cot[PAIR[0, i], rows, :].astype(F32) * proj[0, rows, :]
            for k in range(0 if i < F - 1 else 1, i):
                run = run + cot[PAIR[k, i], rows, :].astype(F32) * proj[k, rows, :]
            vbuf[0, pl.ds(pl.multiple_of(i * 128 + r * 16, 16), 16), :] = run.astype(BF16)

    pl.semaphore_wait(bar, NP - 1 + NZ - 1)

    half = ROWS // NCH

    def zcopy(d, t, c):
        src, dst = (t - 1, t) if d == 0 else ((8 - (t - 1)) % 8, 8 - t)
        rows = pl.ds(c * half, half)
        return pltpu.make_async_remote_copy(
            vbuf.at[src, rows], vbuf.at[dst, rows], zs.at[d, t - 1, c], zr.at[d, t - 1, c],
            device_id=dev(up_z if d == 0 else dn_z, me), device_id_type=MESH,
        )

    def zcopy_wait(d, t, c):
        zcopy(d, t, c).wait_recv()

    for c in range(NCH):
        for d in range(2):
            zcopy(d, 1, c).start()

    def w2copy(r):
        return pltpu.make_async_remote_copy(
            share.at[pl.ds(pl.multiple_of(r * 32, 32), 32)], w2.at[me], ws.at[0], wr.at[0],
            device_id=dev(z, r), device_id_type=MESH,
        )

    @pl.loop(0, NP)
    def _(j):
        r = me ^ j

        @pl.when((r < RED) & (j > 0))
        def _():
            w2copy(r).start()

    loads[3].wait()
    loads[4].wait()
    loads[5].wait()
    hi_iota, lo_iota = iota((512, 128), 0), iota((128, 128), 0)
    for f in range(F):
        t = home[:, f, :]
        table = jnp.concatenate([(t >> 8).astype(F32), (t & 255).astype(F32)], axis=1).astype(BF16)
        idr = ids[f]
        hi, lo = idr >> 7, idr & 127
        oh = jnp.concatenate([onehot(hi_iota == hi[k : k + 1]) for k in range(BAG)], axis=1)
        out = dot(table, oh, 0, 0)
        for k in range(BAG):
            mask = lo_iota == lo[k : k + 1]
            cols = slice(k * 128, k * 128 + 128)
            row = f * BAG + k
            own[row : row + 1, :] = jnp.sum(jnp.where(mask, out[:128, cols], 0.0), axis=0, keepdims=True).astype(I32)
            loc[row : row + 1, :] = jnp.sum(jnp.where(mask, out[128:, cols], 0.0), axis=0, keepdims=True)
            live[row : row + 1, :] = jnp.where(lens[f : f + 1, :] > k, float(f + 1), 0.0)

    upper_tri = jnp.concatenate(
        [onehot(iota((256, 256), 0) < iota((256, 256), 1)), jnp.ones((256, 128), BF16)], axis=1
    )
    own_iota = iota((256, 256), 0)
    o4_iota, rr_iota = iota((64, 256), 0), iota((128, 256), 0)
    lane = (iota((1, 256), 1) % 128).astype(F32)

    def rank_block(j, carry):
        before, table = carry
        two = lambda ref: jnp.concatenate([ref[pl.ds(2 * j, 1), :], ref[pl.ds(2 * j + 1, 1), :]], axis=1)
        o = two(own)
        hit = own_iota == o
        res = dot(onehot(hit), upper_tri)
        ahead = res[:, :256] + jnp.concatenate([before, before], axis=1)
        rank = jnp.sum(jnp.where(hit, ahead, 0.0), axis=0, keepdims=True).astype(I32)
        spot = rr_iota == (o & 3) * CAP + rank
        pay = [jnp.where(spot, v, 0.0).astype(BF16) for v in (lane, two(live), two(loc))]
        table = table + dot(onehot(o4_iota == (o >> 2)), jnp.concatenate(pay, axis=0), 1, 1)
        return before + res[:, 256:], table

    _, table = lax.fori_loop(0, 16, rank_block, (jnp.zeros((256, 128), F32), jnp.zeros((64, 384), F32)))
    m4[...] = (table[:, :128] + 128.0 * table[:, 128:256] + 2048.0 * table[:, 256:]).astype(I32)
    mall[0] = m4[pl.ds(pl.multiple_of(z * 8, 8), 8), :]

    def mcopy(t):
        to = (z + t) % NZ
        return pltpu.make_async_remote_copy(
            m4.at[pl.ds(pl.multiple_of(to * 8, 8), 8)], mall.at[t], ms, mr, device_id=dev(to, me), device_id_type=MESH
        )

    @pl.loop(1, NZ)
    def _(t):
        mcopy(t).start()

    lane128 = iota((128, 128), 1)

    def gather(idx):
        for pq in range(8):
            row = mall[idx, pl.ds(pq, 1), :] & 2047
            col = jnp.broadcast_to(row, (128, 128)).T
            g = jnp.concatenate([onehot(col == lane128 + 128 * (f + 1)) for f in range(F)], axis=1)
            rows = dot(g, vbuf[idx]).astype(BF16)
            stage[idx, pl.ds(pq * 4, 4)] = rows.reshape(4, CAP, D)

    def xycopy(idx, q):
        return pltpu.make_async_remote_copy(
            stage.at[idx, q], got.at[idx, me], ss.at[idx], rr.at[idx], device_id=dev(z, q), device_id_type=MESH
        )

    def send(idx):
        got[idx, me] = stage[idx, me]

        @pl.loop(1, NP)
        def _(j):
            xycopy(idx, me ^ j).start()

    q_iota = iota((256, 128), 0)

    def accumulate(idx):
        peers = got.at[idx, pl.ds(0, NP - 1)]
        pltpu.make_async_copy(peers, peers, rr.at[idx]).wait()
        code = cbuf[idx]
        fcode = (code >> 7) & 15
        lcode = code >> 11
        for g in range(8):
            fcol = jnp.broadcast_to(fcode[g : g + 1, :].astype(F32), (128, 128)).T.astype(BF16)
            v = got[idx, pl.ds(g * 4, 4)].reshape(128, D)
            rows = pl.ds(g * 128, 128)
            for f in range(F):
                bmat[rows, f * D : f * D + D] = jnp.where(fcol == jnp.asarray(f + 1, BF16), v, jnp.zeros_like(v))
            amat[:, g * 128 : g * 128 + 128] = onehot(q_iota == lcode[g : g + 1, :])
        acc_o[...] += dot(amat[...], bmat[...])

    def dcopy(q):
        return pltpu.make_async_remote_copy(
            dsend.at[q], drecv.at[me], ds_, dr, device_id=dev(z, q), device_id_type=MESH
        )

    def targets_out():
        many = mall.at[pl.ds(1, NZ - 1)]
        pltpu.make_async_copy(many, many, mr).wait()
        mine = iota((8, 128), 1) // CAP == me % 4
        for pq in range(8):
            x = mall[:, pq, :]
            for s in range(4):
                y = pltpu.roll(x, s * CAP, 1) if s else x
                dsend[pq * 4 + (me % 4 + 4 - s) % 4] = jnp.where(mine, y, 0)
        drecv[me] = dsend[me]

        @pl.loop(1, NP)
        def _(j):
            dcopy(me ^ j).start()

    def targets_in():
        many = drecv.at[pl.ds(0, NP - 1)]
        pltpu.make_async_copy(many, many, dr).wait()
        for g in range(8):
            cbuf[:, g, :] = drecv[4 * g] + drecv[4 * g + 1] + drecv[4 * g + 2] + drecv[4 * g + 3]

    def w3copy(t):
        return pltpu.make_async_remote_copy(
            part, w3.at[z], ws.at[1], wr.at[1], device_id=dev((z + t) % NZ, me), device_id_type=MESH
        )

    def w4copy(q):
        return pltpu.make_async_remote_copy(
            w4.at[me], w4.at[me], ws.at[2], wr.at[2], device_id=dev(z, q), device_id_type=MESH
        )

    def weight_add():
        @pl.when(me < RED)
        def _():
            peers = w2.at[pl.ds(0, NP - 1)]
            w2[me] = share[pl.ds(pl.multiple_of(me * 32, 32), 32), :]
            pltpu.make_async_copy(peers, peers, wr.at[0]).wait()
            total = w2[0].astype(F32)
            for i in range(1, NP):
                total = total + w2[i].astype(F32)
            part[...] = total
            w3[z] = total

            @pl.loop(1, NZ)
            def _(t):
                w3copy(t).start()

    def weight_spread():
        @pl.when(me < RED)
        def _():
            peers = w3.at[pl.ds(0, NZ - 1)]
            pltpu.make_async_copy(peers, peers, wr.at[1]).wait()
            total = w3[0]
            for i in range(1, NZ):
                total = total + w3[i]
            w4[me] = total.astype(BF16)

            @pl.loop(1, NP)
            def _(j):
                w4copy(me ^ j).start()

    def at(n):
        return jnp.where(n == 7, 4, jnp.where(n % 2 == 1, (n + 1) // 2, (8 - n // 2) % 8))

    acc_o[...] = jnp.zeros_like(acc_o)

    @pl.loop(0, 9)
    def _(n):
        t = (n + 1) // 2

        @pl.when((n % 2 == 1) & (n < 7))
        def _():
            for c in range(NCH):
                for d in range(2):
                    zcopy_wait(d, t, c)

                    @pl.when((t < 3) | ((c < NCH // 2) == (d == 0)))
                    def _():
                        zcopy(d, t + 1, c).start()

        @pl.when(n == 7)
        def _():
            for c in range(NCH // 2):
                zcopy_wait(0, 4, c)
                zcopy_wait(1, 4, c + NCH // 2)

        @pl.when(n == 1)
        def _():
            targets_out()
            weight_add()

        @pl.when(n < 8)
        def _():
            gather(at(n))
            send(at(n))

        @pl.when(n == 2)
        def _():
            targets_in()

        @pl.when(n == 4)
        def _():
            weight_spread()

        @pl.when(n >= 2)
        def _():
            accumulate(at(n - 1))

        @pl.when(n == 2)
        def _():
            accumulate(0)

    @pl.when(me < RED)
    def _():
        peers = w4.at[pl.ds(0, RED - 1)]
        pltpu.make_async_copy(peers, peers, wr.at[2]).wait()

    @pl.when(me >= RED)
    def _():
        pltpu.make_async_copy(w4, w4, wr.at[2]).wait()

    wg_o[...] = w4[...]
    for t in range(1, 5):
        for d in range(2):
            for c in range(NCH):
                if t < 4 or (c < NCH // 2) == (d == 0):
                    zcopy(d, t, c).wait_send()
    many = mall.at[pl.ds(0, NZ - 1)]
    pltpu.make_async_copy(many, many, ms).wait()
    many = dsend.at[pl.ds(0, NP - 1)]
    pltpu.make_async_copy(many, many, ds_).wait()
    for k in range(8):
        many = stage.at[k, pl.ds(0, NP - 1)]
        pltpu.make_async_copy(many, many, ss.at[k]).wait()

    @pl.when(me < RED)
    def _():
        many = w2.at[pl.ds(0, RED - 1)]
        pltpu.make_async_copy(many, many, ws.at[0]).wait()
        many = w3.at[pl.ds(0, NZ - 1)]
        pltpu.make_async_copy(many, many, ws.at[1]).wait()
        many = w2.at[pl.ds(0, NP - 1)]
        pltpu.make_async_copy(many, many, ws.at[2]).wait()

    @pl.when(me >= RED)
    def _():
        many = w2.at[pl.ds(0, RED)]
        pltpu.make_async_copy(many, many, ws.at[0]).wait()


def on_device(pooled, cotangent, bilinear, bag_ids, bag_lens, row_home):
    any_ = pl.BlockSpec(memory_space=pl.ANY)
    vm = pl.BlockSpec(memory_space=pltpu.VMEM)
    dma = pltpu.SemaphoreType.DMA
    wg, acc = pl.pallas_call(
        body,
        out_shape=(
            jax.ShapeDtypeStruct((RED, 32, D), BF16),
            jax.ShapeDtypeStruct((256, F * D), F32),
        ),
        in_specs=[any_] * 6,
        out_specs=(vm, vm),
        scratch_shapes=[
            pltpu.VMEM((ROWS, D), BF16),
            pltpu.VMEM((28, TOK, D), BF16),
            pltpu.VMEM((F - 1, D, D), BF16),
            pltpu.VMEM((F, BAG, TOK), I32),
            pltpu.VMEM((F, TOK), I32),
            pltpu.VMEM((512, F, 128), I32),
            pltpu.VMEM((F, TOK, D), BF16),
            pltpu.VMEM((F - 1, TOK, D), BF16),
            pltpu.VMEM((F - 1, TOK, D), F32),
            pltpu.VMEM((F - 1, TOK, D), F32),
            pltpu.VMEM(((F - 1) * D, D), BF16),
            pltpu.VMEM((F * BAG, 128), I32),
            pltpu.VMEM((F * BAG, 128), F32),
            pltpu.VMEM((F * BAG, 128), F32),
            pltpu.VMEM((64, 128), I32),
            pltpu.VMEM((NZ, 8, 128), I32),
            pltpu.VMEM((NP, 8, 128), I32),
            pltpu.VMEM((NP, 8, 128), I32),
            pltpu.VMEM((NZ, 8, 128), I32),
            pltpu.VMEM((NZ, ROWS, D), BF16),
            pltpu.VMEM((NZ, NP, CAP, D), BF16),
            pltpu.VMEM((NZ, NP, CAP, D), BF16),
            pltpu.VMEM((256, 1024), BF16),
            pltpu.VMEM((1024, F * D), BF16),
            pltpu.VMEM((NP, 32, D), BF16),
            pltpu.VMEM((NZ, 32, D), F32),
            pltpu.VMEM((RED, 32, D), BF16),
            pltpu.VMEM((32, D), F32),
            dma((6,)),
            dma((2, 4, NCH)),
            dma((2, 4, NCH)),
            dma,
            dma,
            dma,
            dma,
            dma((8,)),
            dma((8,)),
            dma((3,)),
            dma((3,)),
        ],
        compiler_params=pltpu.CompilerParams(
            collective_id=0, has_side_effects=True, vmem_limit_bytes=60 * 2**20
        ),
    )(
        pooled.reshape(ROWS, D),
        cotangent.transpose(1, 0, 2),
        bilinear,
        bag_ids.transpose(1, 2, 0),
        bag_lens.transpose(1, 0),
        row_home.reshape(F, 512, 128).transpose(1, 0, 2),
    )
    return wg.reshape(F - 1, D, D).astype(F32), acc.reshape(256, F, D)


def solution(mesh):
    placed = (
        P(("gx", "gy"), None, None),
        P(("gx", "gy"), None, None),
        P(),
        P(("gx", "gy"), None, None),
        P(("gx", "gy"), None),
        P(),
    )
    return jax.shard_map(
        on_device,
        mesh=mesh,
        in_specs=placed,
        out_specs=(P(), P(("gx", "gy"), None, None)),
        check_vma=False,
    )
```

```python
import functools

import jax
import jax.numpy as jnp
from jax import lax
from jax.experimental import pallas as pl
from jax.experimental.pallas import tpu as pltpu
from jax.sharding import PartitionSpec as P

MESH = pl.DeviceIdType.MESH
F = 8
BAG = 4
D = 128
TOK = 128
CAP = 32
NZ = 8
NP = 32
ROWS = F * TOK
NCH = 2
RED = 28
PAIR = {(i, j): p for p, (i, j) in enumerate((i, j) for i in range(F) for j in range(i + 1, F))}
F32, BF16, I32, I16 = jnp.float32, jnp.bfloat16, jnp.int32, jnp.int16


def dev(z, p):
    return (2 * z + p // 16, p % 16)


def iota(shape, dim):
    return lax.broadcasted_iota(I32, shape, dim)


def bf(x):
    return x.astype(F32).astype(BF16)


def onehot(mask):
    return jnp.where(mask, jnp.ones((), BF16), jnp.zeros((), BF16))


def only(mask, x):
    return jnp.where(mask, x, jnp.zeros((), BF16))


def colsum(x):
    acc = x[:16]
    for i in range(16, x.shape[0], 16):
        acc = acc + x[i : i + 16]
    return jnp.sum(acc.astype(F32), axis=0, keepdims=True)


def dot(a, b, ca=1, cb=0):
    return lax.dot_general(a, b, (((ca,), (cb,)), ((), ())), preferred_element_type=F32)


def body(
    pool_h, cot_h, bil_h, ids_h, lens_h, home_h,
    wg_o, acc_o,
    pool, cot, bil, ids, lens, home,
    pf, up, proj, back, share,
    own, loc, live, m4, mall, dsend, drecv, cbuf,
    vbuf, stage, got,
    w2, w3, w4, part,
    lsem, zs, zr, ms, mr, ds_, dr, ss, rr, ws, wr,
):
    gx, gy = lax.axis_index("gx"), lax.axis_index("gy")
    z, me = gx // 2, (gx % 2) * 16 + gy
    up_z, dn_z = (z + 1) % NZ, (z + 7) % NZ

    loads = [
        pltpu.make_async_copy(a, b, lsem.at[n])
        for n, (a, b) in enumerate(
            [(pool_h, pool), (bil_h, bil), (cot_h, cot), (ids_h, ids), (lens_h, lens), (home_h, home)]
        )
    ]
    for c in loads:
        c.start()

    bar = pltpu.get_barrier_semaphore()

    @pl.loop(1, NP)
    def _(j):
        pl.semaphore_signal(bar, inc=1, device_id=dev(z, me ^ j), device_id_type=MESH)

    @pl.loop(1, NZ)
    def _(t):
        pl.semaphore_signal(bar, inc=1, device_id=dev((z + t) % NZ, me), device_id_type=MESH)

    with jax.named_scope("perm"):
        loads[0].wait()
        perm = jnp.where(iota((128, 128), 1) == (iota((128, 128), 0) % 16) * F + iota((128, 128), 0) // 16, 1.0, 0.0).astype(BF16)
        x = jnp.concatenate([pool[pl.ds(g * 128, 128), :] for g in range(8)], axis=1)
        y = dot(perm, x).astype(BF16)
        for g in range(8):
            for f in range(F):
                pf[f, pl.ds(g * 16, 16), :] = y[f * 16 : f * 16 + 16, g * 128 : g * 128 + 128]
    with jax.named_scope("proj"):
        loads[1].wait()
        for i in range(F - 1):
            proj[i] = dot(pf[i], bil[i])
        loads[2].wait()

    with jax.named_scope("upper"):
        @pl.loop(0, 8)
        def _(r):
            rows = pl.ds(pl.multiple_of(r * 16, 16), 16)
            pj = [pf[j, rows, :].astype(F32) for j in range(F)]
            for i in range(F - 1):
                run = cot[PAIR[i, i + 1], rows, :].astype(F32) * pj[i + 1]
                for j in range(i + 2, F):
                    run = run + cot[PAIR[i, j], rows, :].astype(F32) * pj[j]
                up[i, rows, :] = run.astype(BF16)

    with jax.named_scope("mm"):
        for i in range(F - 1):
            back[i] = dot(up[i], bil[i], 1, 1)
        for i in range(F - 1):
            share[pl.ds(i * 128, 128), :] = dot(pf[i], up[i], 0, 0).astype(BF16)

    with jax.named_scope("fgrad"):
        @pl.loop(0, 8)
        def _(r):
            rows = pl.ds(pl.multiple_of(r * 16, 16), 16)
            for i in range(F):
                run = back[i, rows, :] if i < F - 1 else cot[PAIR[0, i], rows, :].astype(F32) * proj[0, rows, :]
                for k in range(0 if i < F - 1 else 1, i):
                    run = run + cot[PAIR[k, i], rows, :].astype(F32) * proj[k, rows, :]
                vbuf[0, pl.ds(pl.multiple_of(i * 128 + r * 16, 16), 16), :] = run.astype(BF16)

    with jax.named_scope("barrier"):
        pl.semaphore_wait(bar, NP - 1 + NZ - 1)

    half = ROWS // NCH

    def zcopy(d, t, c):
        src, dst = (t - 1, t) if d == 0 else ((8 - (t - 1)) % 8, 8 - t)
        rows = pl.ds(c * half, half)
        return pltpu.make_async_remote_copy(
            vbuf.at[src, rows], vbuf.at[dst, rows], zs.at[d, t - 1, c], zr.at[d, t - 1, c],
            device_id=dev(up_z if d == 0 else dn_z, me), device_id_type=MESH,
        )

    with jax.named_scope("zstart"):
        for c in range(NCH):
            for d in range(2):
                zcopy(d, 1, c).start()

    def w2copy(r):
        return pltpu.make_async_remote_copy(
            share.at[pl.ds(pl.multiple_of(r * 32, 32), 32)], w2.at[me], ws.at[0], wr.at[0],
            device_id=dev(z, r), device_id_type=MESH,
        )

    with jax.named_scope("w2start"):
        @pl.loop(0, NP)
        def _(j):
            r = me ^ j

            @pl.when((r < RED) & (j > 0))
            def _():
                w2copy(r).start()

    with jax.named_scope("lookup"):
        loads[3].wait()
        loads[4].wait()
        loads[5].wait()
        hi_iota, lo_iota = iota((512, 128), 0).astype(I16), bf(iota((128, 128), 0))
        for f in range(F):
            t = home[pl.ds(f, 512, stride=F), :].T
            table = bf(jnp.concatenate([t >> 8, t & 255], axis=0))
            hi, lo = (ids[f] >> 7).astype(I16), bf(ids[f] & 127)
            oh = jnp.concatenate([onehot(hi_iota == hi[k : k + 1]) for k in range(BAG)], axis=1)
            out = dot(table, oh).astype(BF16)
            for k in range(BAG):
                mask = lo_iota == lo[k : k + 1]
                cols = slice(k * 128, k * 128 + 128)
                row = f * BAG + k
                own[row : row + 1, :] = colsum(only(mask, out[:128, cols])).astype(I32)
                loc[row : row + 1, :] = colsum(only(mask, out[128:, cols]))
                live[row : row + 1, :] = jnp.where(lens[f : f + 1, :] > k, float(f + 1), 0.0)

    with jax.named_scope("rank"):
        tri = jnp.where(iota((256, 256), 0) < iota((256, 256), 1), 1.0, 0.0).astype(BF16)
        tri = jnp.concatenate([tri, jnp.ones((256, 128), BF16)], axis=1)
        own_iota, o4_iota, rr_iota = bf(iota((256, 128), 0)), bf(iota((64, 128), 0)), bf(iota((128, 128), 0))
        lane = bf(iota((1, 128), 1) + 1)
        o = own[...]
        o_b, o4_b, oc_b = bf(o), bf(o >> 2), bf((o & 3) * CAP)
        loc_b, live_b = loc[...].astype(BF16), live[...].astype(BF16)
        before = jnp.zeros((256, 128), BF16)
        table, lhs, rhs = jnp.zeros((128, 256), F32), [], []
        for j in range(16):
            hit = [own_iota == o_b[r : r + 1] for r in (2 * j, 2 * j + 1)]
            res = dot(jnp.concatenate([onehot(h) for h in hit], axis=1), tri).astype(BF16)
            for n in range(2):
                r = slice(2 * j + n, 2 * j + n + 1)
                rank = colsum(only(hit[n], res[:, n * 128 : n * 128 + 128] + before))
                spot = rr_iota == oc_b[r] + rank.astype(BF16)
                four = o4_iota == o4_b[r]
                rhs.append(jnp.concatenate([only(spot, lane), only(spot, loc_b[r])], axis=0))
                lhs.append(jnp.concatenate([onehot(four), only(four, live_b[r])], axis=0))
            before = before + res[:, 256:]
            if j % 4 == 3:
                table = table + dot(jnp.concatenate(lhs, axis=1), jnp.concatenate(rhs, axis=1), 1, 1)
                lhs, rhs = [], []
        b1 = table[:64, :128]
        f1 = jnp.round(table[64:, :128] / jnp.maximum(b1, 1.0))
        m4[...] = jnp.where(b1 > 0, (b1 - 1.0) + 128.0 * f1 + 2048.0 * table[:64, 128:], 0.0).astype(I32)
    mall[0] = m4[pl.ds(pl.multiple_of(z * 8, 8), 8), :]

    def mcopy(t):
        to = (z + t) % NZ
        return pltpu.make_async_remote_copy(
            m4.at[pl.ds(pl.multiple_of(to * 8, 8), 8)], mall.at[t], ms, mr, device_id=dev(to, me), device_id_type=MESH
        )

    @pl.loop(1, NZ)
    def _(t):
        mcopy(t).start()

    lane128 = iota((128, 128), 1).astype(I16)

    def gather(idx):
        for pq in range(8):
            row = mall[idx, pl.ds(pq, 1), :] & 2047
            col = jnp.broadcast_to(row, (128, 128)).T.astype(I16)
            g = jnp.concatenate([onehot(col == lane128 + jnp.asarray(128 * (f + 1), I16)) for f in range(F)], axis=1)
            rows = dot(g, vbuf[idx]).astype(BF16)
            stage[idx, pl.ds(pq * 4, 4)] = rows.reshape(4, CAP, D)

    def xycopy(idx, q):
        return pltpu.make_async_remote_copy(
            stage.at[idx, q], got.at[idx, me], ss.at[idx], rr.at[idx], device_id=dev(z, q), device_id_type=MESH
        )

    def send(idx):
        got[idx, me] = stage[idx, me]

        @pl.loop(1, NP)
        def _(j):
            xycopy(idx, me ^ j).start()

    q_iota = bf(iota((256, 128), 0))

    def accumulate(idx):
        peers = got.at[idx, pl.ds(0, NP - 1)]
        with jax.named_scope("waitxy"):
            pltpu.make_async_copy(peers, peers, rr.at[idx]).wait()
        code = cbuf[idx]
        field, local = ((code >> 7) & 15).astype(F32), bf(code >> 11)
        lhs, rhs = [], []
        for g in range(8):
            fcol = jnp.broadcast_to(field[g : g + 1, :], (128, 128)).T.astype(BF16)
            v = got[idx, pl.ds(g * 4, 4)].reshape(128, D)
            rhs.append(jnp.concatenate([only(fcol == jnp.asarray(f + 1, BF16), v) for f in range(F)], axis=1))
            lhs.append(onehot(q_iota == local[g : g + 1, :]))
            if g % 4 == 3:
                acc_o[...] += dot(jnp.concatenate(lhs, axis=1), jnp.concatenate(rhs, axis=0))
                lhs, rhs = [], []

    def dcopy(q):
        return pltpu.make_async_remote_copy(
            dsend.at[q], drecv.at[me], ds_, dr, device_id=dev(z, q), device_id_type=MESH
        )

    def targets_out():
        mine = iota((8, 128), 1) // CAP == me % 4
        for pq in range(8):
            x = mall[:, pq, :]
            for s in range(4):
                y = pltpu.roll(x, s * CAP, 1) if s else x
                dsend[pq * 4 + (me % 4 + 4 - s) % 4] = jnp.where(mine, y, 0)
        drecv[me] = dsend[me]

        @pl.loop(1, NP)
        def _(j):
            dcopy(me ^ j).start()

    def targets_in():
        many = drecv.at[pl.ds(0, NP - 1)]
        pltpu.make_async_copy(many, many, dr).wait()
        for g in range(8):
            cbuf[:, g, :] = drecv[4 * g] + drecv[4 * g + 1] + drecv[4 * g + 2] + drecv[4 * g + 3]

    def w3copy(t):
        return pltpu.make_async_remote_copy(
            part, w3.at[z], ws.at[1], wr.at[1], device_id=dev((z + t) % NZ, me), device_id_type=MESH
        )

    def w4copy(q):
        return pltpu.make_async_remote_copy(
            w4.at[me], w4.at[me], ws.at[2], wr.at[2], device_id=dev(z, q), device_id_type=MESH
        )

    def weight_add():
        @pl.when(me < RED)
        def _():
            peers = w2.at[pl.ds(0, NP - 1)]
            w2[me] = share[pl.ds(pl.multiple_of(me * 32, 32), 32), :]
            pltpu.make_async_copy(peers, peers, wr.at[0]).wait()
            total = w2[0].astype(F32)
            for i in range(1, NP):
                total = total + w2[i].astype(F32)
            part[...] = total
            w3[z] = total

            @pl.loop(1, NZ)
            def _(t):
                w3copy(t).start()

    def weight_spread():
        @pl.when(me < RED)
        def _():
            peers = w3.at[pl.ds(0, NZ - 1)]
            pltpu.make_async_copy(peers, peers, wr.at[1]).wait()
            total = w3[0]
            for i in range(1, NZ):
                total = total + w3[i]
            w4[me] = total.astype(BF16)

            @pl.loop(1, NP)
            def _(j):
                w4copy(me ^ j).start()

    def at(n):
        return jnp.where(n == 7, 4, jnp.where(n % 2 == 1, (n + 1) // 2, (8 - n // 2) % 8))

    acc_o[...] = jnp.zeros_like(acc_o)

    def pass_on(t, c):
        for d in range(2):
            with jax.named_scope("waitz"):
                zcopy(d, t, c).wait_recv()

            @pl.when((t < 3) | ((c < NCH // 2) == (d == 0)))
            def _():
                zcopy(d, t + 1, c).start()

    @pl.loop(0, 9)
    def _(n):
        t = (n + 1) // 2

        @pl.when((n % 2 == 1) & (n < 7))
        def _():
            for c in range(NCH // 2, NCH):
                pass_on(t, c)

        @pl.when(n == 7)
        def _():
            for c in range(NCH // 2):
                zcopy(0, 4, c).wait_recv()
                zcopy(1, 4, c + NCH // 2).wait_recv()

        @pl.when(n < 8)
        def _():
            @pl.when(n == 1)
            def _():
                with jax.named_scope("waitm"):
                    many = mall.at[pl.ds(1, NZ - 1)]
                    pltpu.make_async_copy(many, many, mr).wait()

            with jax.named_scope("gather"):
                gather(at(n))
            with jax.named_scope("send"):
                send(at(n))

        @pl.when((n % 2 == 0) & (n < 6))
        def _():
            for c in range(NCH // 2):
                pass_on(t + 1, c)

        @pl.when(n == 2)
        def _():
            with jax.named_scope("targets_out"):
                targets_out()
            with jax.named_scope("weight_add"):
                weight_add()

        @pl.when(n == 4)
        def _():
            with jax.named_scope("targets_in"):
                targets_in()

        @pl.when(n == 5)
        def _():
            with jax.named_scope("weight_spread"):
                weight_spread()

        first = jnp.where(n <= 4, 0, jnp.where(n <= 6, n - 4, jnp.where(n == 7, 4, 5)))
        last = jnp.where(n < 4, 0, jnp.where(n <= 5, n - 3, jnp.where(n == 6, 4, jnp.where(n == 7, 5, 8))))

        @pl.loop(first, last)
        def _(m):
            with jax.named_scope("acc"):
                accumulate(at(m))

    @pl.when(me < RED)
    def _():
        peers = w4.at[pl.ds(0, RED - 1)]
        pltpu.make_async_copy(peers, peers, wr.at[2]).wait()

    @pl.when(me >= RED)
    def _():
        pltpu.make_async_copy(w4, w4, wr.at[2]).wait()

    wg_o[...] = w4[...]
    for t in range(1, 5):
        for d in range(2):
            for c in range(NCH):
                if t < 4 or (c < NCH // 2) == (d == 0):
                    zcopy(d, t, c).wait_send()
    many = mall.at[pl.ds(0, NZ - 1)]
    pltpu.make_async_copy(many, many, ms).wait()
    many = dsend.at[pl.ds(0, NP - 1)]
    pltpu.make_async_copy(many, many, ds_).wait()
    for k in range(8):
        many = stage.at[k, pl.ds(0, NP - 1)]
        pltpu.make_async_copy(many, many, ss.at[k]).wait()

    @pl.when(me < RED)
    def _():
        many = w2.at[pl.ds(0, RED - 1)]
        pltpu.make_async_copy(many, many, ws.at[0]).wait()
        many = w3.at[pl.ds(0, NZ - 1)]
        pltpu.make_async_copy(many, many, ws.at[1]).wait()
        many = w2.at[pl.ds(0, NP - 1)]
        pltpu.make_async_copy(many, many, ws.at[2]).wait()

    @pl.when(me >= RED)
    def _():
        many = w2.at[pl.ds(0, RED)]
        pltpu.make_async_copy(many, many, ws.at[0]).wait()


def on_device(pooled, cotangent, bilinear, bag_ids, bag_lens, row_home):
    any_ = pl.BlockSpec(memory_space=pl.ANY)
    vm = pl.BlockSpec(memory_space=pltpu.VMEM)
    dma = pltpu.SemaphoreType.DMA
    wg, acc = pl.pallas_call(
        body,
        out_shape=(
            jax.ShapeDtypeStruct((RED, 32, D), BF16),
            jax.ShapeDtypeStruct((256, F * D), F32),
        ),
        in_specs=[any_] * 6,
        out_specs=(vm, vm),
        scratch_shapes=[
            pltpu.VMEM((ROWS, D), BF16),
            pltpu.VMEM((28, TOK, D), BF16),
            pltpu.VMEM((F - 1, D, D), BF16),
            pltpu.VMEM((F, BAG, TOK), I32),
            pltpu.VMEM((F, TOK), I32),
            pltpu.VMEM((512 * F, 128), I32),
            pltpu.VMEM((F, TOK, D), BF16),
            pltpu.VMEM((F - 1, TOK, D), BF16),
            pltpu.VMEM((F - 1, TOK, D), F32),
            pltpu.VMEM((F - 1, TOK, D), F32),
            pltpu.VMEM(((F - 1) * D, D), BF16),
            pltpu.VMEM((F * BAG, 128), I32),
            pltpu.VMEM((F * BAG, 128), F32),
            pltpu.VMEM((F * BAG, 128), F32),
            pltpu.VMEM((64, 128), I32),
            pltpu.VMEM((NZ, 8, 128), I32),
            pltpu.VMEM((NP, 8, 128), I32),
            pltpu.VMEM((NP, 8, 128), I32),
            pltpu.VMEM((NZ, 8, 128), I32),
            pltpu.VMEM((NZ, ROWS, D), BF16),
            pltpu.VMEM((NZ, NP, CAP, D), BF16),
            pltpu.VMEM((NZ, NP, CAP, D), BF16),
            pltpu.VMEM((NP, 32, D), BF16),
            pltpu.VMEM((NZ, 32, D), F32),
            pltpu.VMEM((RED, 32, D), BF16),
            pltpu.VMEM((32, D), F32),
            dma((6,)),
            dma((2, 4, NCH)),
            dma((2, 4, NCH)),
            dma,
            dma,
            dma,
            dma,
            dma((8,)),
            dma((8,)),
            dma((3,)),
            dma((3,)),
        ],
        compiler_params=pltpu.CompilerParams(
            collective_id=0, has_side_effects=True, vmem_limit_bytes=60 * 2**20
        ),
    )(
        pooled.reshape(ROWS, D),
        cotangent.transpose(1, 0, 2),
        bilinear,
        bag_ids.transpose(1, 2, 0),
        bag_lens.transpose(1, 0),
        row_home.reshape(F, 512, 128).transpose(1, 0, 2).reshape(512 * F, 128),
    )
    return wg.reshape(F - 1, D, D).astype(F32), acc.reshape(256, F, D)


def solution(mesh):
    placed = (
        P(("gx", "gy"), None, None),
        P(("gx", "gy"), None, None),
        P(),
        P(("gx", "gy"), None, None),
        P(("gx", "gy"), None),
        P(),
    )
    return jax.shard_map(
        on_device,
        mesh=mesh,
        in_specs=placed,
        out_specs=(P(), P(("gx", "gy"), None, None)),
        check_vma=False,
    )
```

```python
import functools

import jax
import jax.numpy as jnp
from jax import lax
from jax.experimental import pallas as pl
from jax.experimental.pallas import tpu as pltpu
from jax.sharding import PartitionSpec as P

MESH = pl.DeviceIdType.MESH
F = 8
BAG = 4
D = 128
TOK = 128
CAP = 32
NZ = 8
NP = 32
ROWS = F * TOK
NCH = 2
RED = 28
PAIR = {(i, j): p for p, (i, j) in enumerate((i, j) for i in range(F) for j in range(i + 1, F))}
F32, BF16, I32, I16 = jnp.float32, jnp.bfloat16, jnp.int32, jnp.int16


def dev(z, p):
    return (2 * z + p // 16, p % 16)


def iota(shape, dim):
    return lax.broadcasted_iota(I32, shape, dim)


def bf(x):
    return x.astype(F32).astype(BF16)


def onehot(mask):
    return jnp.where(mask, jnp.ones((), BF16), jnp.zeros((), BF16))


def only(mask, x):
    return jnp.where(mask, x, jnp.zeros((), BF16))


def colsum(x):
    acc = x[:16]
    for i in range(16, x.shape[0], 16):
        acc = acc + x[i : i + 16]
    return jnp.sum(acc.astype(F32), axis=0, keepdims=True)


def dot(a, b, ca=1, cb=0):
    return lax.dot_general(a, b, (((ca,), (cb,)), ((), ())), preferred_element_type=F32)


def wait_all(ref, sem):
    pltpu.make_async_copy(ref, ref, sem).wait()


def add_slots(code, rows, acc):
    field, local = (code & 15).astype(F32), bf(code >> 4)
    q_iota = bf(iota((256, 128), 0))
    lhs, rhs = [], []
    for g in range(8):
        fcol = jnp.broadcast_to(field[g : g + 1, :], (128, 128)).T.astype(BF16)
        v = rows[pl.ds(g * 4, 4)].reshape(128, D)
        rhs.append(jnp.concatenate([only(fcol == jnp.asarray(f + 1, BF16), v) for f in range(F)], axis=1))
        lhs.append(onehot(q_iota == local[g : g + 1, :]))
        if g % 4 == 3:
            acc[...] += dot(jnp.concatenate(lhs, axis=1), jnp.concatenate(rhs, axis=0))
            lhs, rhs = [], []


def finish(acc_h, got_h, code_h, w4_h, wg_o, tab_o, acc, got, code, w4, wg, part, table, sem):
    loads = [pltpu.make_async_copy(a, b, sem.at[n]) for n, (a, b) in enumerate([(got_h, got), (code_h, code), (w4_h, w4), (acc_h, acc)])]
    for c in loads:
        c.start()
    part[...] = jnp.zeros_like(part)
    loads[0].wait()
    loads[1].wait()
    add_slots(code[...], got, part)
    loads[2].wait()
    wg[...] = w4[...].astype(F32)
    wg_out = pltpu.make_async_copy(wg, wg_o, sem.at[4])
    wg_out.start()
    loads[3].wait()
    for f in range(F):
        cols = slice(f * D, f * D + D)
        table[pl.ds(f, 256, stride=F), :] = acc[:, cols] + part[:, cols]
    table_out = pltpu.make_async_copy(table, tab_o, sem.at[5])
    table_out.start()
    wg_out.wait()
    table_out.wait()


def body(
    pool_h, cot_h, bil_h, ids_h, lens_h, home_h,
    acc_o, got_o, code_o, w4_o,
    pool, cot, bil, ids, lens, home,
    pf, up, proj, back, share,
    own, loc, live, m4, mall, dsend, drecv, cbuf,
    vbuf, stage, got,
    acc, w2, w3, w4, part, done,
    lsem, zs, zr, ms, mr, ds_, dr, ss, rr, ws, wr,
):
    gx, gy = lax.axis_index("gx"), lax.axis_index("gy")
    z, me = gx // 2, (gx % 2) * 16 + gy
    up_z, dn_z = (z + 1) % NZ, (z + 7) % NZ

    loads = [
        pltpu.make_async_copy(a, b, lsem.at[n])
        for n, (a, b) in enumerate(
            [(pool_h, pool), (bil_h, bil), (cot_h, cot), (ids_h, ids), (lens_h, lens), (home_h, home)]
        )
    ]
    for c in loads:
        c.start()

    bar = pltpu.get_barrier_semaphore()

    @pl.loop(1, NP)
    def _(j):
        pl.semaphore_signal(bar, inc=1, device_id=dev(z, me ^ j), device_id_type=MESH)

    @pl.loop(1, NZ)
    def _(t):
        pl.semaphore_signal(bar, inc=1, device_id=dev((z + t) % NZ, me), device_id_type=MESH)

    with jax.named_scope("perm"):
        loads[0].wait()
        perm = jnp.where(iota((128, 128), 1) == (iota((128, 128), 0) % 16) * F + iota((128, 128), 0) // 16, 1.0, 0.0).astype(BF16)
        x = jnp.concatenate([pool[pl.ds(g * 128, 128), :] for g in range(8)], axis=1)
        y = dot(perm, x).astype(BF16)
        for g in range(8):
            for f in range(F):
                pf[f, pl.ds(g * 16, 16), :] = y[f * 16 : f * 16 + 16, g * 128 : g * 128 + 128]
    with jax.named_scope("proj"):
        loads[1].wait()
        for i in range(F - 1):
            proj[i] = dot(pf[i], bil[i])
        loads[2].wait()

    with jax.named_scope("upper"):
        @pl.loop(0, 8)
        def _(r):
            rows = pl.ds(pl.multiple_of(r * 16, 16), 16)
            pj = [pf[j, rows, :].astype(F32) for j in range(F)]
            for i in range(F - 1):
                run = cot[PAIR[i, i + 1], rows, :].astype(F32) * pj[i + 1]
                for j in range(i + 2, F):
                    run = run + cot[PAIR[i, j], rows, :].astype(F32) * pj[j]
                up[i, rows, :] = run.astype(BF16)

    with jax.named_scope("mm"):
        for i in range(F - 1):
            back[i] = dot(up[i], bil[i], 1, 1)
        for i in range(F - 1):
            share[pl.ds(i * 128, 128), :] = dot(pf[i], up[i], 0, 0).astype(BF16)

    with jax.named_scope("fgrad"):
        @pl.loop(0, 8)
        def _(r):
            rows = pl.ds(pl.multiple_of(r * 16, 16), 16)
            for i in range(F):
                run = back[i, rows, :] if i < F - 1 else cot[PAIR[0, i], rows, :].astype(F32) * proj[0, rows, :]
                for k in range(0 if i < F - 1 else 1, i):
                    run = run + cot[PAIR[k, i], rows, :].astype(F32) * proj[k, rows, :]
                vbuf[0, pl.ds(pl.multiple_of(i * 128 + r * 16, 16), 16), :] = run.astype(BF16)

    with jax.named_scope("lookup"):
        loads[3].wait()
        loads[4].wait()
        loads[5].wait()
        hi_iota, lo_iota = iota((512, 128), 0).astype(I16), bf(iota((128, 128), 0))
        for f in range(F):
            t = home[pl.ds(f, 512, stride=F), :].T
            table = bf(jnp.concatenate([t >> 8, t & 255], axis=0))
            hi, lo = (ids[f] >> 7).astype(I16), bf(ids[f] & 127)
            oh = jnp.concatenate([onehot(hi_iota == hi[k : k + 1]) for k in range(BAG)], axis=1)
            out = dot(table, oh).astype(BF16)
            for k in range(BAG):
                mask = lo_iota == lo[k : k + 1]
                cols = slice(k * 128, k * 128 + 128)
                row = f * BAG + k
                own[row : row + 1, :] = colsum(only(mask, out[:128, cols])).astype(I32)
                loc[row : row + 1, :] = colsum(only(mask, out[128:, cols]))
                live[row : row + 1, :] = jnp.where(lens[f : f + 1, :] > k, float(f + 1), 0.0)

    with jax.named_scope("barrier"):
        pl.semaphore_wait(bar, NP - 1 + NZ - 1)

    half = ROWS // NCH

    def zcopy(d, t, c):
        src, dst = (t - 1, t) if d == 0 else ((8 - (t - 1)) % 8, 8 - t)
        rows = pl.ds(c * half, half)
        return pltpu.make_async_remote_copy(
            vbuf.at[src, rows], vbuf.at[dst, rows], zs.at[d, t - 1, c], zr.at[d, t - 1, c],
            device_id=dev(up_z if d == 0 else dn_z, me), device_id_type=MESH,
        )

    def first_hop(pieces):
        for c in pieces:
            for d in range(2):
                zcopy(d, 1, c).start()

    first_hop(range(NCH // 2))

    def w2copy(r):
        return pltpu.make_async_remote_copy(
            share.at[pl.ds(pl.multiple_of(r * 32, 32), 32)], w2.at[me], ws.at[0], wr.at[0],
            device_id=dev(z, r), device_id_type=MESH,
        )

    def shares_out():
        @pl.loop(0, NP)
        def _(j):
            r = me ^ j

            @pl.when((r < RED) & (j > 0))
            def _():
                w2copy(r).start()

    with jax.named_scope("shares_out"):
        shares_out()

    with jax.named_scope("rank"):
        tri = jnp.where(iota((256, 256), 0) < iota((256, 256), 1), 1.0, 0.0).astype(BF16)
        tri = jnp.concatenate([tri, jnp.ones((256, 128), BF16)], axis=1)
        own_iota, o4_iota, rr_iota = bf(iota((256, 128), 0)), bf(iota((64, 128), 0)), bf(iota((128, 128), 0))
        lane = bf(iota((1, 128), 1) + 1)
        o = own[...]
        o_b, o4_b, oc_b = bf(o), bf(o >> 2), bf((o & 3) * CAP)
        loc_b, live_b = loc[...].astype(BF16), live[...].astype(BF16)
        before = jnp.zeros((256, 128), BF16)
        table, lhs, rhs = jnp.zeros((128, 256), F32), [], []
        for j in range(16):
            hit = [own_iota == o_b[r : r + 1] for r in (2 * j, 2 * j + 1)]
            res = dot(jnp.concatenate([onehot(h) for h in hit], axis=1), tri).astype(BF16)
            for n in range(2):
                r = slice(2 * j + n, 2 * j + n + 1)
                rank = colsum(only(hit[n], res[:, n * 128 : n * 128 + 128] + before))
                spot = rr_iota == oc_b[r] + rank.astype(BF16)
                four = o4_iota == o4_b[r]
                rhs.append(jnp.concatenate([only(spot, lane), only(spot, loc_b[r])], axis=0))
                lhs.append(jnp.concatenate([onehot(four), only(four, live_b[r])], axis=0))
            before = before + res[:, 256:]
            if j % 4 == 3:
                table = table + dot(jnp.concatenate(lhs, axis=1), jnp.concatenate(rhs, axis=1), 1, 1)
                lhs, rhs = [], []
        b1 = table[:64, :128]
        f1 = jnp.round(table[64:, :128] / jnp.maximum(b1, 1.0))
        m4[...] = jnp.where(b1 > 0, (b1 - 1.0) + 128.0 * f1 + 2048.0 * table[:64, 128:], 0.0).astype(I32)
    mall[0] = m4[pl.ds(pl.multiple_of(z * 8, 8), 8), :]

    def mcopy(t):
        to = (z + t) % NZ
        return pltpu.make_async_remote_copy(
            m4.at[pl.ds(pl.multiple_of(to * 8, 8), 8)], mall.at[t], ms, mr.at[t], device_id=dev(to, me), device_id_type=MESH
        )

    @pl.loop(1, NZ)
    def _(t):
        mcopy(t).start()

    first_hop(range(NCH // 2, NCH))

    lane128 = iota((128, 128), 1).astype(I16)

    def gather(idx):
        for pq in range(8):
            row = mall[idx, pl.ds(pq, 1), :] & 2047
            col = jnp.broadcast_to(row, (128, 128)).T.astype(I16)
            g = jnp.concatenate([onehot(col == lane128 + jnp.asarray(128 * (f + 1), I16)) for f in range(F)], axis=1)
            rows = dot(g, vbuf[idx]).astype(BF16)
            stage[idx, pl.ds(pq * 4, 4)] = rows.reshape(4, CAP, D)

    def xycopy(idx, q):
        return pltpu.make_async_remote_copy(
            stage.at[idx, q], got.at[idx, me], ss.at[idx], rr.at[idx], device_id=dev(z, q), device_id_type=MESH
        )

    def send(idx):
        got[idx, me] = stage[idx, me]

        @pl.loop(1, NP)
        def _(j):
            xycopy(idx, me ^ j).start()

    def last_own():
        return pltpu.make_async_copy(stage.at[4, me], got_o.at[me], lsem.at[6])

    def send_last():
        last_own().start()

        @pl.loop(1, NP)
        def _(j):
            pltpu.make_async_remote_copy(
                stage.at[4, me ^ j], got_o.at[me], ss.at[4], rr.at[4], device_id=dev(z, me ^ j), device_id_type=MESH
            ).start()

    def accumulate(idx):
        with jax.named_scope("waitxy"):
            wait_all(got.at[idx, pl.ds(0, NP - 1)], rr.at[idx])
        add_slots(cbuf[idx], got.at[idx], acc)

    def dcopy(q):
        return pltpu.make_async_remote_copy(
            dsend.at[q], drecv.at[me], ds_, dr, device_id=dev(z, q), device_id_type=MESH
        )

    def targets_out():
        for t in range(2, NZ - 1):
            mcopy(t).wait_recv()
        mine = iota((8, 128), 1) // CAP == me % 4
        for pq in range(8):
            x = mall[:, pq, :] >> 7
            for s in range(4):
                y = pltpu.roll(x, s * CAP, 1) if s else x
                dsend[pq * 4 + (me % 4 + 4 - s) % 4] = jnp.where(mine, y, 0).astype(I16)
        drecv[me] = dsend[me]

        @pl.loop(1, NP)
        def _(j):
            dcopy(me ^ j).start()

    def targets_in():
        many = drecv.at[pl.ds(0, NP - 1)]
        pltpu.make_async_copy(many, many, dr).wait()
        for g in range(8):
            cbuf[:, g, :] = sum(drecv[4 * g + n].astype(I32) for n in range(4))

    def w3copy(t):
        to = (z + t) % NZ
        return pltpu.make_async_remote_copy(
            part.at[to], w3.at[z], ws.at[1], wr.at[1], device_id=dev(to, me), device_id_type=MESH
        )

    def w3back(t):
        return pltpu.make_async_remote_copy(
            done.at[z], done.at[z], ws.at[2], wr.at[2], device_id=dev((z + t) % NZ, me), device_id_type=MESH
        )

    def w4copy(q):
        mine = w4.at[me // 2, me % 2]
        return pltpu.make_async_remote_copy(
            mine, mine, ws.at[3], wr.at[3], device_id=dev(z, q), device_id_type=MESH
        )

    def w4side():
        mine = w4.at[:, me % 2]
        return pltpu.make_async_remote_copy(
            mine, mine, ws.at[4], wr.at[4], device_id=dev(z, me ^ 1), device_id_type=MESH
        )

    adder = me < RED

    def weight_add():
        @pl.when(adder)
        def _():
            w2[me] = share[pl.ds(pl.multiple_of(me * 32, 32), 32), :]
            wait_all(w2.at[pl.ds(0, NP - 1)], wr.at[0])
            total = w2[0].astype(F32)
            for i in range(1, NP):
                total = total + w2[i].astype(F32)
            part[...] = total.reshape(NZ, 4, D)
            w3[z] = part[z]

            @pl.loop(1, NZ)
            def _(t):
                w3copy(t).start()

    def weight_column():
        @pl.when(adder)
        def _():
            wait_all(w3.at[pl.ds(0, NZ - 1)], wr.at[1])
            total = w3[0]
            for i in range(1, NZ):
                total = total + w3[i]
            done[z] = total

            @pl.loop(1, NZ)
            def _(t):
                w3back(t).start()

    def weight_spread():
        @pl.when(adder)
        def _():
            wait_all(done.at[pl.ds(0, NZ - 1)], wr.at[2])
            w4[me // 2, me % 2] = done[...].reshape(32, D).astype(BF16)

            @pl.loop(1, NP // 2)
            def _(j):
                w4copy(me ^ (2 * j)).start()

    def weight_side():
        @pl.when(adder)
        def _():
            wait_all(w4.at[pl.ds(0, RED // 2 - 1), 0], wr.at[3])

        @pl.when(me >= RED)
        def _():
            wait_all(w4.at[:, 0], wr.at[3])

        w4side().start()

    def at(n):
        return jnp.where(n == 7, 4, jnp.where(n % 2 == 1, (n + 1) // 2, (8 - n // 2) % 8))

    acc[...] = jnp.zeros_like(acc)

    def pass_on(t, c):
        for d in range(2):
            with jax.named_scope("waitz"):
                zcopy(d, t, c).wait_recv()

            @pl.when((t < 3) | ((c < NCH // 2) == (d == 0)))
            def _():
                zcopy(d, t + 1, c).start()

    @pl.loop(0, 9)
    def _(n):
        t = (n + 1) // 2

        @pl.when((n % 2 == 1) & (n < 7))
        def _():
            for c in range(NCH // 2, NCH):
                pass_on(t, c)

        @pl.when(n == 7)
        def _():
            for c in range(NCH // 2):
                zcopy(0, 4, c).wait_recv()
                zcopy(1, 4, c + NCH // 2).wait_recv()

        @pl.when(n < 8)
        def _():
            @pl.when((n == 1) | (n == 2))
            def _():
                with jax.named_scope("waitm"):
                    mcopy(at(n)).wait_recv()

            with jax.named_scope("gather"):
                gather(at(n))

            @pl.when(n < 7)
            def _():
                with jax.named_scope("send"):
                    send(at(n))

            @pl.when(n == 7)
            def _():
                with jax.named_scope("send"):
                    send_last()


        @pl.when((n % 2 == 0) & (n < 6))
        def _():
            for c in range(NCH // 2):
                pass_on(t + 1, c)

        @pl.when(n == 2)
        def _():
            with jax.named_scope("targets_out"):
                targets_out()

        @pl.when(n == 1)
        def _():
            with jax.named_scope("weight_add"):
                weight_add()

        @pl.when(n == 3)
        def _():
            with jax.named_scope("weight_column"):
                weight_column()

        @pl.when(n == 4)
        def _():
            with jax.named_scope("targets_in"):
                targets_in()

        @pl.when(n == 5)
        def _():
            with jax.named_scope("weight_spread"):
                weight_spread()

        @pl.when(n == 8)
        def _():
            with jax.named_scope("weight_side"):
                weight_side()

        first = jnp.where(n <= 4, 0, jnp.where(n <= 6, n - 4, jnp.where(n == 7, 4, 5)))
        last = jnp.where(n < 4, 0, jnp.where(n <= 5, n - 3, jnp.where(n == 6, 4, jnp.where(n == 7, 5, 7))))

        @pl.loop(first, last)
        def _(m):
            with jax.named_scope("acc"):
                accumulate(at(m))

    w4side().wait()
    outs = [
        pltpu.make_async_copy(a, b, lsem.at[n])
        for n, (a, b) in enumerate([(acc, acc_o), (cbuf.at[4], code_o), (w4, w4_o)])
    ]
    for c in outs:
        c.start()
    for t in range(1, 5):
        for d in range(2):
            for c in range(NCH):
                if t < 4 or (c < NCH // 2) == (d == 0):
                    zcopy(d, t, c).wait_send()
    wait_all(mall.at[pl.ds(0, NZ - 1)], ms)
    wait_all(dsend.at[pl.ds(0, NP - 1)], ds_)
    for k in range(8):
        wait_all(stage.at[k, pl.ds(0, NP - 1)], ss.at[k])

    @pl.when(adder)
    def _():
        wait_all(w2.at[pl.ds(0, RED - 1)], ws.at[0])
        wait_all(w3.at[pl.ds(0, NZ - 1)], ws.at[1])
        wait_all(done.at[pl.ds(0, NZ - 1)], ws.at[2])
        wait_all(w2.at[pl.ds(0, NP // 2 - 1)], ws.at[3])

    @pl.when(me >= RED)
    def _():
        wait_all(w2.at[pl.ds(0, RED)], ws.at[0])

    for c in outs:
        c.wait()
    last_own().wait()
    with jax.named_scope("waitxy"):
        wait_all(got_o.at[pl.ds(0, NP - 1)], rr.at[4])


def on_device(pooled, cotangent, bilinear, bag_ids, bag_lens, row_home):
    any_ = pl.BlockSpec(memory_space=pl.ANY)
    dma = pltpu.SemaphoreType.DMA
    acc, got, code, w4 = pl.pallas_call(
        body,
        out_shape=(
            jax.ShapeDtypeStruct((256, F * D), F32),
            jax.ShapeDtypeStruct((NP, CAP, D), BF16),
            jax.ShapeDtypeStruct((8, 128), I32),
            jax.ShapeDtypeStruct((RED // 2, 2, 32, D), BF16),
        ),
        in_specs=[any_] * 6,
        out_specs=[any_] * 4,
        scratch_shapes=[
            pltpu.VMEM((ROWS, D), BF16),
            pltpu.VMEM((28, TOK, D), BF16),
            pltpu.VMEM((F - 1, D, D), BF16),
            pltpu.VMEM((F, BAG, TOK), I32),
            pltpu.VMEM((F, TOK), I32),
            pltpu.VMEM((512 * F, 128), I32),
            pltpu.VMEM((F, TOK, D), BF16),
            pltpu.VMEM((F - 1, TOK, D), BF16),
            pltpu.VMEM((F - 1, TOK, D), F32),
            pltpu.VMEM((F - 1, TOK, D), F32),
            pltpu.VMEM(((F - 1) * D, D), BF16),
            pltpu.VMEM((F * BAG, 128), I32),
            pltpu.VMEM((F * BAG, 128), F32),
            pltpu.VMEM((F * BAG, 128), F32),
            pltpu.VMEM((64, 128), I32),
            pltpu.VMEM((NZ, 8, 128), I32),
            pltpu.VMEM((NP, 8, 128), I16),
            pltpu.VMEM((NP, 8, 128), I16),
            pltpu.VMEM((NZ, 8, 128), I32),
            pltpu.VMEM((NZ, ROWS, D), BF16),
            pltpu.VMEM((NZ, NP, CAP, D), BF16),
            pltpu.VMEM((NZ, NP, CAP, D), BF16),
            pltpu.VMEM((256, F * D), F32),
            pltpu.VMEM((NP, 32, D), BF16),
            pltpu.VMEM((NZ, 4, D), F32),
            pltpu.VMEM((RED // 2, 2, 32, D), BF16),
            pltpu.VMEM((NZ, 4, D), F32),
            pltpu.VMEM((NZ, 4, D), F32),
            dma((7,)),
            dma((2, 4, NCH)),
            dma((2, 4, NCH)),
            dma,
            dma((NZ,)),
            dma,
            dma,
            dma((8,)),
            dma((8,)),
            dma((5,)),
            dma((5,)),
        ],
        compiler_params=pltpu.CompilerParams(
            collective_id=0, has_side_effects=True, vmem_limit_bytes=60 * 2**20
        ),
    )(
        pooled.reshape(ROWS, D),
        cotangent.transpose(1, 0, 2),
        bilinear,
        bag_ids.transpose(1, 2, 0),
        bag_lens.transpose(1, 0),
        row_home.reshape(F, 512, 128).transpose(1, 0, 2).reshape(512 * F, 128),
    )
    wg, table = pl.pallas_call(
        finish,
        out_shape=(
            jax.ShapeDtypeStruct(((F - 1) * D, D), F32),
            jax.ShapeDtypeStruct((256 * F, D), F32),
        ),
        in_specs=[any_] * 4,
        out_specs=[any_] * 2,
        scratch_shapes=[
            pltpu.VMEM((256, F * D), F32),
            pltpu.VMEM((NP, CAP, D), BF16),
            pltpu.VMEM((8, 128), I32),
            pltpu.VMEM(((F - 1) * D, D), BF16),
            pltpu.VMEM(((F - 1) * D, D), F32),
            pltpu.VMEM((256, F * D), F32),
            pltpu.VMEM((256 * F, D), F32),
            dma((6,)),
        ],
        compiler_params=pltpu.CompilerParams(vmem_limit_bytes=60 * 2**20),
    )(acc, got, code, w4.reshape((F - 1) * D, D))
    return wg.reshape(F - 1, D, D), table.reshape(256, F, D)


def solution(mesh):
    placed = (
        P(("gx", "gy"), None, None),
        P(("gx", "gy"), None, None),
        P(),
        P(("gx", "gy"), None, None),
        P(("gx", "gy"), None),
        P(),
    )
    return jax.shard_map(
        on_device,
        mesh=mesh,
        in_specs=placed,
        out_specs=(P(), P(("gx", "gy"), None, None)),
        check_vma=False,
    )
```

```python
import functools

import jax
import jax.numpy as jnp
from jax import lax
from jax.experimental import pallas as pl
from jax.experimental.pallas import tpu as pltpu
from jax.sharding import PartitionSpec as P

MESH = pl.DeviceIdType.MESH
F = 8
BAG = 4
D = 128
TOK = 128
CAP = 32
NZ = 8
NP = 32
ROWS = F * TOK
NCH = 4
RED = 28
PAIR = {(i, j): p for p, (i, j) in enumerate((i, j) for i in range(F) for j in range(i + 1, F))}
F32, BF16, I32, I16 = jnp.float32, jnp.bfloat16, jnp.int32, jnp.int16


def dev(z, p):
    return (2 * z + p // 16, p % 16)


def iota(shape, dim):
    return lax.broadcasted_iota(I32, shape, dim)


def bf(x):
    return x.astype(F32).astype(BF16)


def onehot(mask):
    return jnp.where(mask, jnp.ones((), BF16), jnp.zeros((), BF16))


def only(mask, x):
    return jnp.where(mask, x, jnp.zeros((), BF16))


def colsum(x):
    acc = x[:16]
    for i in range(16, x.shape[0], 16):
        acc = acc + x[i : i + 16]
    return jnp.sum(acc.astype(F32), axis=0, keepdims=True)


def dot(a, b, ca=1, cb=0):
    return lax.dot_general(a, b, (((ca,), (cb,)), ((), ())), preferred_element_type=F32)


def wait_all(ref, sem):
    pltpu.make_async_copy(ref, ref, sem).wait()


def add_slots(code, rows, acc):
    field, local = (code & 15).astype(F32), bf(code >> 4)
    q_iota = bf(iota((256, 128), 0))
    lhs, rhs = [], []
    for g in range(8):
        fcol = jnp.broadcast_to(field[g : g + 1, :], (128, 128)).T.astype(BF16)
        v = rows[pl.ds(g * 4, 4)].reshape(128, D)
        rhs.append(jnp.concatenate([only(fcol == jnp.asarray(f + 1, BF16), v) for f in range(F)], axis=1))
        lhs.append(onehot(q_iota == local[g : g + 1, :]))
        if g % 4 == 3:
            acc[...] += dot(jnp.concatenate(lhs, axis=1), jnp.concatenate(rhs, axis=0))
            lhs, rhs = [], []


def finish(acc_h, got_h, code_h, w4_h, wg_o, tab_o, acc, got, code, w4, wg, part, table, sem):
    loads = [pltpu.make_async_copy(a, b, sem.at[n]) for n, (a, b) in enumerate([(got_h, got), (code_h, code), (w4_h, w4), (acc_h, acc)])]
    for c in loads:
        c.start()
    part[...] = jnp.zeros_like(part)
    loads[0].wait()
    loads[1].wait()
    add_slots(code[...], got, part)
    loads[2].wait()
    wg[...] = w4[...].astype(F32)
    wg_out = pltpu.make_async_copy(wg, wg_o, sem.at[4])
    wg_out.start()
    loads[3].wait()
    for f in range(F):
        cols = slice(f * D, f * D + D)
        table[pl.ds(f, 256, stride=F), :] = acc[:, cols] + part[:, cols]
    table_out = pltpu.make_async_copy(table, tab_o, sem.at[5])
    table_out.start()
    wg_out.wait()
    table_out.wait()


def body(
    pool_h, cot_h, bil_h, ids_h, lens_h, home_h,
    acc_o, got_o, code_o, w4_o,
    pool, cot, bil, ids, lens, home,
    pf, up, proj, back, share,
    own, loc, live, m4, mall, dsend, drecv, cbuf,
    vbuf, stage, got,
    acc, w2, w3, w4, part, done,
    lsem, zs, zr, ms, mr, ds_, dr, ss, rr, ws, wr,
):
    gx, gy = lax.axis_index("gx"), lax.axis_index("gy")
    z, me = gx // 2, (gx % 2) * 16 + gy
    core = gy % 2

    loads = [
        pltpu.make_async_copy(a, b, lsem.at[n])
        for n, (a, b) in enumerate(
            [(pool_h, pool), (bil_h, bil), (cot_h, cot), (ids_h, ids), (lens_h, lens), (home_h, home)]
        )
    ]
    for c in loads:
        c.start()

    bar = pltpu.get_barrier_semaphore()

    @pl.loop(1, NP)
    def _(j):
        pl.semaphore_signal(bar, inc=1, device_id=dev(z, me ^ j), device_id_type=MESH)

    @pl.loop(1, NZ)
    def _(t):
        pl.semaphore_signal(bar, inc=1, device_id=dev((z + t) % NZ, me), device_id_type=MESH)

    with jax.named_scope("perm"):
        loads[0].wait()
        perm = jnp.where(iota((128, 128), 1) == (iota((128, 128), 0) % 16) * F + iota((128, 128), 0) // 16, 1.0, 0.0).astype(BF16)
        x = jnp.concatenate([pool[pl.ds(g * 128, 128), :] for g in range(8)], axis=1)
        y = dot(perm, x).astype(BF16)
        for g in range(8):
            for f in range(F):
                pf[f, pl.ds(g * 16, 16), :] = y[f * 16 : f * 16 + 16, g * 128 : g * 128 + 128]
    with jax.named_scope("proj"):
        loads[1].wait()
        for i in range(F - 1):
            proj[i] = dot(pf[i], bil[i])
        loads[2].wait()

    with jax.named_scope("upper"):
        @pl.loop(0, 8)
        def _(r):
            rows = pl.ds(pl.multiple_of(r * 16, 16), 16)
            pj = [pf[j, rows, :].astype(F32) for j in range(F)]
            for i in range(F - 1):
                run = cot[PAIR[i, i + 1], rows, :].astype(F32) * pj[i + 1]
                for j in range(i + 2, F):
                    run = run + cot[PAIR[i, j], rows, :].astype(F32) * pj[j]
                up[i, rows, :] = run.astype(BF16)

    with jax.named_scope("mm"):
        for i in range(F - 1):
            back[i] = dot(up[i], bil[i], 1, 1)
        for i in range(F - 1):
            share[pl.ds(i * 128, 128), :] = dot(pf[i], up[i], 0, 0).astype(BF16)

    with jax.named_scope("fgrad"):
        @pl.loop(0, 8)
        def _(r):
            rows = pl.ds(pl.multiple_of(r * 16, 16), 16)
            for i in range(F):
                run = back[i, rows, :] if i < F - 1 else cot[PAIR[0, i], rows, :].astype(F32) * proj[0, rows, :]
                for k in range(0 if i < F - 1 else 1, i):
                    run = run + cot[PAIR[k, i], rows, :].astype(F32) * proj[k, rows, :]
                vbuf[0, pl.ds(pl.multiple_of(i * 128 + r * 16, 16), 16), :] = run.astype(BF16)

    with jax.named_scope("barrier"):
        pl.semaphore_wait(bar, NP - 1 + NZ - 1)

    piece = ROWS // NCH

    def zcopy(e, t, c):
        src = jnp.where(t == 1, 0, 2 * t - 3 + e)
        dst = jnp.where(t == 4, 7, 2 * t - 1 + e)
        at = jnp.where(e == 0, c, NCH - 1 - c)
        rows = pl.ds(pl.multiple_of(at * piece, piece), piece)
        to = (z + jnp.where(e == core, 1, NZ - 1)) % NZ
        return pltpu.make_async_remote_copy(
            vbuf.at[src, rows], vbuf.at[dst, rows], zs.at[e, t - 1, c], zr.at[e, t - 1, c],
            device_id=dev(to, me), device_id_type=MESH,
        )

    def first_hop(e):
        for c in range(NCH):
            zcopy(e, 1, c).start()

    first_hop(0)

    def w2copy(r):
        return pltpu.make_async_remote_copy(
            share.at[pl.ds(pl.multiple_of(r * 32, 32), 32)], w2.at[me], ws.at[0], wr.at[0],
            device_id=dev(z, r), device_id_type=MESH,
        )

    def shares_out():
        @pl.loop(0, NP)
        def _(j):
            r = me ^ j

            @pl.when((r < RED) & (j > 0))
            def _():
                w2copy(r).start()

    with jax.named_scope("shares_out"):
        shares_out()

    with jax.named_scope("lookup"):
        loads[3].wait()
        loads[4].wait()
        loads[5].wait()
        hi_iota, lo_iota = iota((512, 128), 0).astype(I16), bf(iota((128, 128), 0))
        for f in range(F):
            t = home[pl.ds(f, 512, stride=F), :].T
            table = bf(jnp.concatenate([t >> 8, t & 255], axis=0))
            hi, lo = (ids[f] >> 7).astype(I16), bf(ids[f] & 127)
            oh = jnp.concatenate([onehot(hi_iota == hi[k : k + 1]) for k in range(BAG)], axis=1)
            out = dot(table, oh).astype(BF16)
            for k in range(BAG):
                mask = lo_iota == lo[k : k + 1]
                cols = slice(k * 128, k * 128 + 128)
                row = f * BAG + k
                own[row : row + 1, :] = colsum(only(mask, out[:128, cols])).astype(I32)
                loc[row : row + 1, :] = colsum(only(mask, out[128:, cols]))
                live[row : row + 1, :] = jnp.where(lens[f : f + 1, :] > k, float(f + 1), 0.0)

    first_hop(1)

    with jax.named_scope("rank"):
        tri = jnp.where(iota((256, 256), 0) < iota((256, 256), 1), 1.0, 0.0).astype(BF16)
        tri = jnp.concatenate([tri, jnp.ones((256, 128), BF16)], axis=1)
        own_iota, o4_iota, rr_iota = bf(iota((256, 128), 0)), bf(iota((64, 128), 0)), bf(iota((128, 128), 0))
        lane = bf(iota((1, 128), 1) + 1)
        o = own[...]
        o_b, o4_b, oc_b = bf(o), bf(o >> 2), bf((o & 3) * CAP)
        loc_b, live_b = loc[...].astype(BF16), live[...].astype(BF16)
        before = jnp.zeros((256, 128), BF16)
        table, lhs, rhs = jnp.zeros((128, 256), F32), [], []
        for j in range(16):
            hit = [own_iota == o_b[r : r + 1] for r in (2 * j, 2 * j + 1)]
            res = dot(jnp.concatenate([onehot(h) for h in hit], axis=1), tri).astype(BF16)
            for n in range(2):
                r = slice(2 * j + n, 2 * j + n + 1)
                rank = colsum(only(hit[n], res[:, n * 128 : n * 128 + 128] + before))
                spot = rr_iota == oc_b[r] + rank.astype(BF16)
                four = o4_iota == o4_b[r]
                rhs.append(jnp.concatenate([only(spot, lane), only(spot, loc_b[r])], axis=0))
                lhs.append(jnp.concatenate([onehot(four), only(four, live_b[r])], axis=0))
            before = before + res[:, 256:]
            if j % 4 == 3:
                table = table + dot(jnp.concatenate(lhs, axis=1), jnp.concatenate(rhs, axis=1), 1, 1)
                lhs, rhs = [], []
        b1 = table[:64, :128]
        f1 = jnp.round(table[64:, :128] / jnp.maximum(b1, 1.0))
        m4[...] = jnp.where(b1 > 0, (b1 - 1.0) + 128.0 * f1 + 2048.0 * table[:64, 128:], 0.0).astype(I32)
    mall[0] = m4[pl.ds(pl.multiple_of(z * 8, 8), 8), :]

    def mcopy(n):
        t = (n + 1) // 2
        to = (z + jnp.where((n - 1) % 2 == core, t, NZ - t)) % NZ
        return pltpu.make_async_remote_copy(
            m4.at[pl.ds(pl.multiple_of(to * 8, 8), 8)], mall.at[n], ms, mr.at[n], device_id=dev(to, me), device_id_type=MESH
        )

    @pl.loop(1, NZ)
    def _(t):
        mcopy(t).start()


    lane128 = iota((128, 128), 1).astype(I16)

    def gather(idx):
        for pq in range(8):
            row = mall[idx, pl.ds(pq, 1), :] & 2047
            col = jnp.broadcast_to(row, (128, 128)).T.astype(I16)
            g = jnp.concatenate([onehot(col == lane128 + jnp.asarray(128 * (f + 1), I16)) for f in range(F)], axis=1)
            rows = dot(g, vbuf[idx]).astype(BF16)
            stage[idx, pl.ds(pq * 4, 4)] = rows.reshape(4, CAP, D)

    def xycopy(idx, q):
        return pltpu.make_async_remote_copy(
            stage.at[idx, q], got.at[idx, me], ss.at[idx], rr.at[idx], device_id=dev(z, q), device_id_type=MESH
        )

    def send(idx):
        got[idx, me] = stage[idx, me]
        for j in range(1, NP):
            xycopy(idx, me ^ j).start()

    def last_own():
        return pltpu.make_async_copy(stage.at[7, me], got_o.at[me], lsem.at[6])

    def send_last():
        last_own().start()

        @pl.loop(1, NP)
        def _(j):
            pltpu.make_async_remote_copy(
                stage.at[7, me ^ j], got_o.at[me], ss.at[7], rr.at[7], device_id=dev(z, me ^ j), device_id_type=MESH
            ).start()

    def accumulate(idx):
        with jax.named_scope("waitxy"):
            wait_all(got.at[idx, pl.ds(0, NP - 1)], rr.at[idx])
        add_slots(cbuf[idx], got.at[idx], acc)

    def dcopy(q):
        return pltpu.make_async_remote_copy(
            dsend.at[q], drecv.at[me], ds_, dr, device_id=dev(z, q), device_id_type=MESH
        )

    def targets_out():
        for n in range(3, NZ):
            mcopy(n).wait_recv()
        mine = iota((8, 128), 1) // CAP == me % 4
        for pq in range(8):
            x = mall[:, pq, :] >> 7
            for s in range(4):
                y = pltpu.roll(x, s * CAP, 1) if s else x
                dsend[pq * 4 + (me % 4 + 4 - s) % 4] = jnp.where(mine, y, 0).astype(I16)
        drecv[me] = dsend[me]

        @pl.loop(1, NP)
        def _(j):
            dcopy(me ^ j).start()

    def targets_in():
        many = drecv.at[pl.ds(0, NP - 1)]
        pltpu.make_async_copy(many, many, dr).wait()
        for g in range(8):
            cbuf[:, g, :] = sum(drecv[4 * g + n].astype(I32) for n in range(4))

    def w3copy(t):
        to = (z + t) % NZ
        return pltpu.make_async_remote_copy(
            part.at[to], w3.at[z], ws.at[1], wr.at[1], device_id=dev(to, me), device_id_type=MESH
        )

    def w3back(t):
        return pltpu.make_async_remote_copy(
            done.at[z], done.at[z], ws.at[2], wr.at[2], device_id=dev((z + t) % NZ, me), device_id_type=MESH
        )

    def w4copy(q):
        mine = w4.at[me // 2, me % 2]
        return pltpu.make_async_remote_copy(
            mine, mine, ws.at[3], wr.at[3], device_id=dev(z, q), device_id_type=MESH
        )

    def w4side():
        mine = w4.at[:, me % 2]
        return pltpu.make_async_remote_copy(
            mine, mine, ws.at[4], wr.at[4], device_id=dev(z, me ^ 1), device_id_type=MESH
        )

    adder = me < RED

    def weight_add():
        @pl.when(adder)
        def _():
            w2[me] = share[pl.ds(pl.multiple_of(me * 32, 32), 32), :]
            wait_all(w2.at[pl.ds(0, NP - 1)], wr.at[0])
            total = w2[0].astype(F32)
            for i in range(1, NP):
                total = total + w2[i].astype(F32)
            part[...] = total.reshape(NZ, 4, D)
            w3[z] = part[z]

            @pl.loop(1, NZ)
            def _(t):
                w3copy(t).start()

    def weight_column():
        @pl.when(adder)
        def _():
            wait_all(w3.at[pl.ds(0, NZ - 1)], wr.at[1])
            total = w3[0]
            for i in range(1, NZ):
                total = total + w3[i]
            done[z] = total

            @pl.loop(1, NZ)
            def _(t):
                w3back(t).start()

    def weight_spread():
        @pl.when(adder)
        def _():
            wait_all(done.at[pl.ds(0, NZ - 1)], wr.at[2])
            w4[me // 2, me % 2] = done[...].reshape(32, D).astype(BF16)

            @pl.loop(1, NP // 2)
            def _(j):
                w4copy(me ^ (2 * j)).start()

    def weight_side():
        @pl.when(adder)
        def _():
            wait_all(w4.at[pl.ds(0, RED // 2 - 1), 0], wr.at[3])

        @pl.when(me >= RED)
        def _():
            wait_all(w4.at[:, 0], wr.at[3])

        w4side().start()

    acc[...] = jnp.zeros_like(acc)

    def pass_on(n, c):
        e, t = (n - 1) % 2, (n + 1) // 2
        with jax.named_scope(f"waitz{c}"):
            zcopy(e, t, c).wait_recv()

        @pl.when((t < 3) | (c < NCH // 2))
        def _():
            zcopy(e, t + 1, c).start()

    @pl.loop(0, 9)
    def _(n):
        @pl.when((n > 0) & (n < 7))
        def _():
            pass_on(n, 3)

        @pl.when(n == 7)
        def _():
            with jax.named_scope("waitz4"):
                for c in range(NCH // 2):
                    for e in range(2):
                        zcopy(e, 4, c).wait_recv()

        @pl.when(n < 8)
        def _():
            @pl.when((n == 1) | (n == 2))
            def _():
                with jax.named_scope("waitm"):
                    mcopy(n).wait_recv()

            with jax.named_scope("gather"):
                gather(n)

            @pl.when(n < 7)
            def _():
                with jax.named_scope("send"):
                    send(n)

            @pl.when(n == 7)
            def _():
                with jax.named_scope("send"):
                    send_last()


        def once(when, what):
            @pl.when(n == when)
            def _():
                with jax.named_scope(what.__name__):
                    what()

        def add(lo, hi):
            @pl.loop(lo, hi)
            def _(m):
                with jax.named_scope("acc"):
                    accumulate(m)

        @pl.when(n < 6)
        def _():
            pass_on(n + 1, 0)
            pass_on(n + 1, 1)

        once(1, weight_add)
        once(2, targets_out)
        once(3, weight_column)
        once(4, targets_in)
        once(5, weight_spread)
        once(8, weight_side)
        add(jnp.where(n <= 4, 0, n - 4), jnp.where(n < 4, 0, jnp.where(n == 8, 7, n - 3)))

        @pl.when(n < 6)
        def _():
            pass_on(n + 1, 2)

    outs = [pltpu.make_async_copy(acc, acc_o, lsem.at[0]), pltpu.make_async_copy(cbuf.at[7], code_o, lsem.at[1])]
    for c in outs:
        c.start()
    with jax.named_scope("waitside"):
        w4side().wait()
    outs.append(pltpu.make_async_copy(w4, w4_o, lsem.at[2]))
    outs[-1].start()
    for t in range(1, 5):
        for d in range(2):
            for c in range(NCH):
                if t < 4 or c < NCH // 2:
                    zcopy(d, t, c).wait_send()
    wait_all(mall.at[pl.ds(0, NZ - 1)], ms)
    wait_all(dsend.at[pl.ds(0, NP - 1)], ds_)
    for k in range(8):
        wait_all(stage.at[k, pl.ds(0, NP - 1)], ss.at[k])

    @pl.when(adder)
    def _():
        wait_all(w2.at[pl.ds(0, RED - 1)], ws.at[0])
        wait_all(w3.at[pl.ds(0, NZ - 1)], ws.at[1])
        wait_all(done.at[pl.ds(0, NZ - 1)], ws.at[2])
        wait_all(w2.at[pl.ds(0, NP // 2 - 1)], ws.at[3])

    @pl.when(me >= RED)
    def _():
        wait_all(w2.at[pl.ds(0, RED)], ws.at[0])

    for c in outs:
        c.wait()
    last_own().wait()
    with jax.named_scope("waitxy"):
        wait_all(got_o.at[pl.ds(0, NP - 1)], rr.at[7])


def on_device(pooled, cotangent, bilinear, bag_ids, bag_lens, row_home):
    any_ = pl.BlockSpec(memory_space=pl.ANY)
    dma = pltpu.SemaphoreType.DMA
    acc, got, code, w4 = pl.pallas_call(
        body,
        out_shape=(
            jax.ShapeDtypeStruct((256, F * D), F32),
            jax.ShapeDtypeStruct((NP, CAP, D), BF16),
            jax.ShapeDtypeStruct((8, 128), I32),
            jax.ShapeDtypeStruct((RED // 2, 2, 32, D), BF16),
        ),
        in_specs=[any_] * 6,
        out_specs=[any_] * 4,
        scratch_shapes=[
            pltpu.VMEM((ROWS, D), BF16),
            pltpu.VMEM((28, TOK, D), BF16),
            pltpu.VMEM((F - 1, D, D), BF16),
            pltpu.VMEM((F, BAG, TOK), I32),
            pltpu.VMEM((F, TOK), I32),
            pltpu.VMEM((512 * F, 128), I32),
            pltpu.VMEM((F, TOK, D), BF16),
            pltpu.VMEM((F - 1, TOK, D), BF16),
            pltpu.VMEM((F - 1, TOK, D), F32),
            pltpu.VMEM((F - 1, TOK, D), F32),
            pltpu.VMEM(((F - 1) * D, D), BF16),
            pltpu.VMEM((F * BAG, 128), I32),
            pltpu.VMEM((F * BAG, 128), F32),
            pltpu.VMEM((F * BAG, 128), F32),
            pltpu.VMEM((64, 128), I32),
            pltpu.VMEM((NZ, 8, 128), I32),
            pltpu.VMEM((NP, 8, 128), I16),
            pltpu.VMEM((NP, 8, 128), I16),
            pltpu.VMEM((NZ, 8, 128), I32),
            pltpu.VMEM((NZ, ROWS, D), BF16),
            pltpu.VMEM((NZ, NP, CAP, D), BF16),
            pltpu.VMEM((NZ, NP, CAP, D), BF16),
            pltpu.VMEM((256, F * D), F32),
            pltpu.VMEM((NP, 32, D), BF16),
            pltpu.VMEM((NZ, 4, D), F32),
            pltpu.VMEM((RED // 2, 2, 32, D), BF16),
            pltpu.VMEM((NZ, 4, D), F32),
            pltpu.VMEM((NZ, 4, D), F32),
            dma((7,)),
            dma((2, 4, NCH)),
            dma((2, 4, NCH)),
            dma,
            dma((NZ,)),
            dma,
            dma,
            dma((8,)),
            dma((8,)),
            dma((5,)),
            dma((5,)),
        ],
        compiler_params=pltpu.CompilerParams(
            collective_id=0, has_side_effects=True, vmem_limit_bytes=60 * 2**20
        ),
    )(
        pooled.reshape(ROWS, D),
        cotangent.transpose(1, 0, 2),
        bilinear,
        bag_ids.transpose(1, 2, 0),
        bag_lens.transpose(1, 0),
        row_home.reshape(F, 512, 128).transpose(1, 0, 2).reshape(512 * F, 128),
    )
    wg, table = pl.pallas_call(
        finish,
        out_shape=(
            jax.ShapeDtypeStruct(((F - 1) * D, D), F32),
            jax.ShapeDtypeStruct((256 * F, D), F32),
        ),
        in_specs=[any_] * 4,
        out_specs=[any_] * 2,
        scratch_shapes=[
            pltpu.VMEM((256, F * D), F32),
            pltpu.VMEM((NP, CAP, D), BF16),
            pltpu.VMEM((8, 128), I32),
            pltpu.VMEM(((F - 1) * D, D), BF16),
            pltpu.VMEM(((F - 1) * D, D), F32),
            pltpu.VMEM((256, F * D), F32),
            pltpu.VMEM((256 * F, D), F32),
            dma((6,)),
        ],
        compiler_params=pltpu.CompilerParams(vmem_limit_bytes=60 * 2**20),
    )(acc, got, code, w4.reshape((F - 1) * D, D))
    return wg.reshape(F - 1, D, D), table.reshape(256, F, D)


def solution(mesh):
    placed = (
        P(("gx", "gy"), None, None),
        P(("gx", "gy"), None, None),
        P(),
        P(("gx", "gy"), None, None),
        P(("gx", "gy"), None),
        P(),
    )
    return jax.shard_map(
        on_device,
        mesh=mesh,
        in_specs=placed,
        out_specs=(P(), P(("gx", "gy"), None, None)),
        check_vma=False,
    )
```

```python
import functools

import jax
import jax.numpy as jnp
from jax import lax
from jax.experimental import pallas as pl
from jax.experimental.pallas import tpu as pltpu
from jax.sharding import PartitionSpec as P

MESH = pl.DeviceIdType.MESH
F = 8
BAG = 4
D = 128
TOK = 128
CAP = 32
NZ = 8
NP = 32
ROWS = F * TOK
NCH = 4
RED = 28
PAIR = {(i, j): p for p, (i, j) in enumerate((i, j) for i in range(F) for j in range(i + 1, F))}
F32, BF16, I32, I16 = jnp.float32, jnp.bfloat16, jnp.int32, jnp.int16


def dev(z, p):
    return (2 * z + p // 16, p % 16)


def iota(shape, dim):
    return lax.broadcasted_iota(I32, shape, dim)


def bf(x):
    return x.astype(F32).astype(BF16)


def onehot(mask):
    return jnp.where(mask, jnp.ones((), BF16), jnp.zeros((), BF16))


def only(mask, x):
    return jnp.where(mask, x, jnp.zeros((), BF16))


def colsum(x):
    acc = x[:16]
    for i in range(16, x.shape[0], 16):
        acc = acc + x[i : i + 16]
    return jnp.sum(acc.astype(F32), axis=0, keepdims=True)


def dot(a, b, ca=1, cb=0):
    return lax.dot_general(a, b, (((ca,), (cb,)), ((), ())), preferred_element_type=F32)


def wait_all(ref, sem):
    pltpu.make_async_copy(ref, ref, sem).wait()


def add_slots(code, rows, acc):
    field, local = (code & 15).astype(F32), bf(code >> 4)
    q_iota = bf(iota((256, 128), 0))
    lhs, rhs = [], []
    for g in range(8):
        fcol = jnp.broadcast_to(field[g : g + 1, :], (128, 128)).T.astype(BF16)
        v = rows[pl.ds(g * 4, 4)].reshape(128, D)
        rhs.append(jnp.concatenate([only(fcol == jnp.asarray(f + 1, BF16), v) for f in range(F)], axis=1))
        lhs.append(onehot(q_iota == local[g : g + 1, :]))
        if g % 4 == 3:
            acc[...] += dot(jnp.concatenate(lhs, axis=1), jnp.concatenate(rhs, axis=0))
            lhs, rhs = [], []


def finish(acc_h, got_h, code_h, w4_h, wg_o, tab_o, acc, got, code, w4, wg, part, table, sem):
    loads = [pltpu.make_async_copy(a, b, sem.at[n]) for n, (a, b) in enumerate([(got_h, got), (code_h, code), (w4_h, w4), (acc_h, acc)])]
    for c in loads:
        c.start()
    part[...] = jnp.zeros_like(part)
    loads[0].wait()
    loads[1].wait()
    add_slots(code[...], got, part)
    loads[2].wait()
    wg[...] = w4[...].astype(F32)
    wg_out = pltpu.make_async_copy(wg, wg_o, sem.at[4])
    wg_out.start()
    loads[3].wait()
    for f in range(F):
        cols = slice(f * D, f * D + D)
        table[pl.ds(f, 256, stride=F), :] = acc[:, cols] + part[:, cols]
    table_out = pltpu.make_async_copy(table, tab_o, sem.at[5])
    table_out.start()
    wg_out.wait()
    table_out.wait()


def body(
    pool_h, cot_h, bil_h, ids_h, lens_h, home_h,
    acc_o, got_o, code_o, w4_o,
    pool, cot, bil, ids, lens, home,
    pf, up, proj, back, share,
    own, loc, live, m4, mall, dsend, drecv, cbuf,
    vbuf, stage, got,
    acc, w2, w3, w4, part, done,
    lsem, zs, zr, ms, mr, ds_, dr, ss, rr, ws, wr,
):
    gx, gy = lax.axis_index("gx"), lax.axis_index("gy")
    z, me = gx // 2, (gx % 2) * 16 + gy
    core = gy % 2

    loads = [
        pltpu.make_async_copy(a, b, lsem.at[n])
        for n, (a, b) in enumerate(
            [(pool_h, pool), (bil_h, bil), (cot_h, cot), (ids_h, ids), (lens_h, lens), (home_h, home)]
        )
    ]
    for c in loads:
        c.start()

    bar = pltpu.get_barrier_semaphore()

    for t in (4, 3, 5, 2, 6, 1, 7):
        pl.semaphore_signal(bar, inc=1, device_id=dev((z + t) % NZ, me), device_id_type=MESH)
    for j in range(NP - 1, 0, -1):
        pl.semaphore_signal(bar, inc=1, device_id=dev(z, me ^ j), device_id_type=MESH)

    with jax.named_scope("perm"):
        loads[0].wait()
        perm = jnp.where(iota((128, 128), 1) == (iota((128, 128), 0) % 16) * F + iota((128, 128), 0) // 16, 1.0, 0.0).astype(BF16)
        x = jnp.concatenate([pool[pl.ds(g * 128, 128), :] for g in range(8)], axis=1)
        y = dot(perm, x).astype(BF16)
        for g in range(8):
            for f in range(F):
                pf[f, pl.ds(g * 16, 16), :] = y[f * 16 : f * 16 + 16, g * 128 : g * 128 + 128]
    with jax.named_scope("grads"):
        loads[1].wait()
        loads[2].wait()
        for i in range(F - 1):
            proj[i] = dot(pf[i], bil[i])
        for r in range(0, TOK, 16):
            rows = pl.ds(r, 16)
            pj = [pf[j, rows, :].astype(F32) for j in range(F)]
            for i in range(F - 1):
                run = cot[PAIR[i, i + 1], rows, :].astype(F32) * pj[i + 1]
                for j in range(i + 2, F):
                    run = run + cot[PAIR[i, j], rows, :].astype(F32) * pj[j]
                up[i, rows, :] = run.astype(BF16)
        for i in range(F - 1):
            back[i] = dot(up[i], bil[i], 1, 1)
        for r in range(0, TOK, 16):
            rows = pl.ds(r, 16)
            for i in range(F):
                run = back[i, rows, :] if i < F - 1 else cot[PAIR[0, i], rows, :].astype(F32) * proj[0, rows, :]
                for k in range(0 if i < F - 1 else 1, i):
                    run = run + cot[PAIR[k, i], rows, :].astype(F32) * proj[k, rows, :]
                vbuf[0, pl.ds(i * TOK + r, 16), :] = run.astype(BF16)
        for i in range(F - 1):
            share[pl.ds(i * D, D), :] = dot(pf[i], up[i], 0, 0).astype(BF16)

    with jax.named_scope("barrier"):
        pl.semaphore_wait(bar, NP - 1 + NZ - 1)

    piece = ROWS // NCH

    def zcopy(e, t, c):
        src = jnp.where(t == 1, 0, 2 * t - 3 + e)
        dst = jnp.where(t == 4, 7, 2 * t - 1 + e)
        at = jnp.where(e == 0, c, NCH - 1 - c)
        rows = pl.ds(pl.multiple_of(at * piece, piece), piece)
        to = (z + jnp.where(e == core, 1, NZ - 1)) % NZ
        return pltpu.make_async_remote_copy(
            vbuf.at[src, rows], vbuf.at[dst, rows], zs.at[e, t - 1, c], zr.at[e, t - 1, c],
            device_id=dev(to, me), device_id_type=MESH,
        )

    def first_hop(e):
        for c in range(NCH):
            zcopy(e, 1, c).start()

    first_hop(0)

    def w2copy(r):
        return pltpu.make_async_remote_copy(
            share.at[pl.ds(pl.multiple_of(r * 32, 32), 32)], w2.at[me], ws.at[0], wr.at[0],
            device_id=dev(z, r), device_id_type=MESH,
        )

    def shares_out():
        @pl.loop(0, NP)
        def _(j):
            r = me ^ j

            @pl.when((r < RED) & (j > 0))
            def _():
                w2copy(r).start()

    with jax.named_scope("shares_out"):
        shares_out()

    @pl.when(gx >= 0)
    def _():
        with jax.named_scope("lookup"):
            loads[3].wait()
            loads[4].wait()
            loads[5].wait()
            hi_iota, lo_iota = iota((512, 128), 0).astype(I16), bf(iota((128, 128), 0))
            for f in range(F):
                t = home[pl.ds(f, 512, stride=F), :].T
                table = bf(jnp.concatenate([t >> 8, t & 255], axis=0))
                hi, lo = (ids[f] >> 7).astype(I16), bf(ids[f] & 127)
                oh = jnp.concatenate([onehot(hi_iota == hi[k : k + 1]) for k in range(BAG)], axis=1)
                out = dot(table, oh).astype(BF16)
                for k in range(BAG):
                    mask = lo_iota == lo[k : k + 1]
                    cols = slice(k * 128, k * 128 + 128)
                    row = f * BAG + k
                    own[row : row + 1, :] = colsum(only(mask, out[:128, cols])).astype(I32)
                    loc[row : row + 1, :] = colsum(only(mask, out[128:, cols]))
                    live[row : row + 1, :] = jnp.where(lens[f : f + 1, :] > k, float(f + 1), 0.0)

    first_hop(1)

    @pl.when(gx >= 0)
    def _():
        with jax.named_scope("rank"):
            tri = jnp.where(iota((256, 256), 0) <= iota((256, 256), 1), 1.0, 0.0).astype(BF16)
            own_iota, o4_iota, rr_iota = bf(iota((256, 128), 0)), bf(iota((64, 128), 0)), bf(iota((128, 128), 0))
            lane = bf(iota((1, 128), 1) + 1)
            o = own[...]
            o_b, o4_b, oc_b = bf(o), bf(o >> 2), bf((o & 3) * CAP - 1)
            loc_b, live_b = loc[...].astype(BF16), live[...].astype(BF16)
            before = jnp.zeros((256, 128), BF16)
            lhs, rhs = [], []
            for j in range(16):
                hit = [own_iota == o_b[r : r + 1] for r in (2 * j, 2 * j + 1)]
                count = dot(jnp.concatenate([onehot(h) for h in hit], axis=1), tri).astype(BF16)
                for n in range(2):
                    r = slice(2 * j + n, 2 * j + n + 1)
                    rank = colsum(only(hit[n], count[:, n * 128 : n * 128 + 128] + before))
                    spot = rr_iota == oc_b[r] + rank.astype(BF16)
                    four = o4_iota == o4_b[r]
                    lhs.append(jnp.concatenate([only(spot, lane), only(spot, loc_b[r])], axis=0))
                    rhs.append(jnp.concatenate([onehot(four), only(four, live_b[r])], axis=0))
                before = before + jnp.broadcast_to(count[:, 255:], (256, 128))
            table = dot(jnp.concatenate(lhs, axis=1), jnp.concatenate(rhs, axis=1), 1, 1).T
            b1 = table[:64, :128]
            f1 = jnp.round(table[64:, :128] / jnp.maximum(b1, 1.0))
            m4[...] = jnp.where(b1 > 0, (b1 - 1.0) + 128.0 * f1 + 2048.0 * table[:64, 128:], 0.0).astype(I32)
    mall[0] = m4[pl.ds(pl.multiple_of(z * 8, 8), 8), :]

    def mcopy(n):
        t = (n + 1) // 2
        to = (z + jnp.where((n - 1) % 2 == core, t, NZ - t)) % NZ
        return pltpu.make_async_remote_copy(
            m4.at[pl.ds(pl.multiple_of(to * 8, 8), 8)], mall.at[n], ms, mr.at[n], device_id=dev(to, me), device_id_type=MESH
        )

    @pl.loop(1, NZ)
    def _(t):
        mcopy(t).start()


    lane128 = iota((128, 128), 1).astype(I16)

    def gather(idx):
        for pq in range(8):
            row = mall[idx, pl.ds(pq, 1), :] & 2047
            col = jnp.broadcast_to(row, (128, 128)).T.astype(I16)
            g = jnp.concatenate([onehot(col == lane128 + jnp.asarray(128 * (f + 1), I16)) for f in range(F)], axis=1)
            rows = dot(g, vbuf[idx]).astype(BF16)
            stage[idx, pl.ds(pq * 4, 4)] = rows.reshape(4, CAP, D)

    def xycopy(idx, q):
        return pltpu.make_async_remote_copy(
            stage.at[idx, q], got.at[idx, me], ss.at[idx], rr.at[idx], device_id=dev(z, q), device_id_type=MESH
        )

    def send(idx):
        got[idx, me] = stage[idx, me]
        for j in range(1, NP):
            xycopy(idx, me ^ j).start()

    def last_own():
        return pltpu.make_async_copy(stage.at[7, me], got_o.at[me], lsem.at[6])

    def send_last():
        last_own().start()
        for j in range(1, NP):
            pltpu.make_async_remote_copy(
                stage.at[7, me ^ j], got_o.at[me], ss.at[7], rr.at[7], device_id=dev(z, me ^ j), device_id_type=MESH
            ).start()

    def accumulate(idx):
        with jax.named_scope("waitxy"):
            wait_all(got.at[idx, pl.ds(0, NP - 1)], rr.at[idx])
        add_slots(cbuf[idx], got.at[idx], acc)

    def fold(y):
        y = y + pltpu.roll(y, 7, 0)
        return y + pltpu.roll(y, 6, 0)

    def dcopy(q):
        return pltpu.make_async_remote_copy(
            dsend.at[q], drecv.at[me], ds_, dr, device_id=dev(z, q), device_id_type=MESH
        )

    def targets_out():
        for n in range(3, NZ):
            mcopy(n).wait_recv()
        row4, block = iota((8, 128), 0) % 4, iota((8, 128), 1) // CAP
        for pq in range(8):
            x = mall[:, pq, :] >> 7
            turned = [pltpu.roll(x, s * CAP, 1) if s else x for s in range(4)]
            for j in range(4):
                y = sum(jnp.where((block == row4) & ((row4 + 4 - j) % 4 == s), turned[s], 0) for s in range(4))
                y = fold(y)
                dsend[pq * 4 + j] = y[0:1] + (y[4:5] << 16)
        drecv[me] = dsend[me]

        @pl.loop(1, NP)
        def _(j):
            dcopy(me ^ j).start()

    def targets_in():
        many = drecv.at[pl.ds(0, NP - 1)]
        pltpu.make_async_copy(many, many, dr).wait()
        row4, block = iota((8, 128), 0) % 4, iota((8, 128), 1) // CAP
        for v in range(4):
            words = drecv[pl.ds(v * 8, 8)].reshape(8, 128)
            for r in range(2):
                x = (words >> 16) if r else (words & 0xFFFF)
                turned = [pltpu.roll(x, s * CAP, 1) if s else x for s in range(4)]
                for m in range(4):
                    y = sum(jnp.where((block == row4) & ((row4 + 4 - m) % 4 == s), turned[s], 0) for s in range(4))
                    y = fold(y)
                    for h in range(2):
                        cbuf[4 * r + m, 2 * v + h : 2 * v + h + 1, :] = y[4 * h : 4 * h + 1]

    def w3copy(t):
        to = (z + t) % NZ
        return pltpu.make_async_remote_copy(
            part.at[to], w3.at[z], ws.at[1], wr.at[1], device_id=dev(to, me), device_id_type=MESH
        )

    def w3back(t):
        return pltpu.make_async_remote_copy(
            done.at[z], done.at[z], ws.at[2], wr.at[2], device_id=dev((z + t) % NZ, me), device_id_type=MESH
        )

    def w4copy(q):
        mine = w4.at[me // 2, me % 2]
        return pltpu.make_async_remote_copy(
            mine, mine, ws.at[3], wr.at[3], device_id=dev(z, q), device_id_type=MESH
        )

    def w4side():
        mine = w4.at[:, me % 2]
        return pltpu.make_async_remote_copy(
            mine, mine, ws.at[4], wr.at[4], device_id=dev(z, me ^ 1), device_id_type=MESH
        )

    adder = me < RED

    def weight_add():
        @pl.when(adder)
        def _():
            w2[me] = share[pl.ds(pl.multiple_of(me * 32, 32), 32), :]
            wait_all(w2.at[pl.ds(0, NP - 1)], wr.at[0])
            total = w2[0].astype(F32)
            for i in range(1, NP):
                total = total + w2[i].astype(F32)
            part[...] = total.reshape(NZ, 4, D)
            w3[z] = part[z]

            @pl.loop(1, NZ)
            def _(t):
                w3copy(t).start()

    def weight_column():
        @pl.when(adder)
        def _():
            wait_all(w3.at[pl.ds(0, NZ - 1)], wr.at[1])
            total = w3[0]
            for i in range(1, NZ):
                total = total + w3[i]
            done[z] = total

            @pl.loop(1, NZ)
            def _(t):
                w3back(t).start()

    def weight_spread():
        @pl.when(adder)
        def _():
            wait_all(done.at[pl.ds(0, NZ - 1)], wr.at[2])
            w4[me // 2, me % 2] = done[...].reshape(32, D).astype(BF16)

            @pl.loop(1, NP // 2)
            def _(j):
                w4copy(me ^ (2 * j)).start()

    def weight_side():
        @pl.when(adder)
        def _():
            wait_all(w4.at[pl.ds(0, RED // 2 - 1), 0], wr.at[3])

        @pl.when(me >= RED)
        def _():
            wait_all(w4.at[:, 0], wr.at[3])

        w4side().start()

    acc[...] = jnp.zeros_like(acc)

    def pass_on(n, c):
        e, t = (n - 1) % 2, (n + 1) // 2
        with jax.named_scope(f"waitz{c}"):
            zcopy(e, t, c).wait_recv()

        @pl.when((t < 3) | (c < NCH // 2))
        def _():
            zcopy(e, t + 1, c).start()

    @pl.loop(0, 9)
    def _(n):
        @pl.when((n > 0) & (n < 7))
        def _():
            pass_on(n, 2)

            @pl.when(n < 6)
            def _():
                pass_on(n + 1, 0)

            pass_on(n, 3)

        @pl.when(n == 7)
        def _():
            with jax.named_scope("waitz4"):
                for c in range(NCH // 2):
                    for e in range(2):
                        zcopy(e, 4, c).wait_recv()

        @pl.when(n < 8)
        def _():
            @pl.when((n == 1) | (n == 2))
            def _():
                with jax.named_scope("waitm"):
                    mcopy(n).wait_recv()

            with jax.named_scope("gather"):
                gather(n)

            @pl.when(n < 7)
            def _():
                with jax.named_scope("send"):
                    send(n)

            @pl.when(n == 7)
            def _():
                with jax.named_scope("send"):
                    send_last()


        def once(when, what):
            @pl.when(n == when)
            def _():
                with jax.named_scope(what.__name__):
                    what()

        def add(lo, hi):
            @pl.loop(lo, hi)
            def _(m):
                with jax.named_scope("acc"):
                    accumulate(m)

        @pl.when(n == 0)
        def _():
            pass_on(1, 0)

        @pl.when(n < 6)
        def _():
            pass_on(n + 1, 1)

        once(1, weight_add)
        once(2, targets_out)
        once(3, weight_column)
        once(5, targets_in)
        once(5, weight_spread)
        add(jnp.where(n <= 5, 0, 1), jnp.where(n < 5, 0, jnp.where(n == 8, 6, 1)))
        once(8, weight_side)
        add(6, jnp.where(n == 8, 7, 6))

    outs = [pltpu.make_async_copy(acc, acc_o, lsem.at[0]), pltpu.make_async_copy(cbuf.at[7], code_o, lsem.at[1])]
    for c in outs:
        c.start()
    with jax.named_scope("waitside"):
        w4side().wait()
    outs.append(pltpu.make_async_copy(w4, w4_o, lsem.at[2]))
    outs[-1].start()
    for t in range(1, 5):
        for d in range(2):
            for c in range(NCH):
                if t < 4 or c < NCH // 2:
                    zcopy(d, t, c).wait_send()
    wait_all(mall.at[pl.ds(0, NZ - 1)], ms)
    wait_all(dsend.at[pl.ds(0, NP - 1)], ds_)
    for k in range(8):
        wait_all(stage.at[k, pl.ds(0, NP - 1)], ss.at[k])

    @pl.when(adder)
    def _():
        wait_all(w2.at[pl.ds(0, RED - 1)], ws.at[0])
        wait_all(w3.at[pl.ds(0, NZ - 1)], ws.at[1])
        wait_all(done.at[pl.ds(0, NZ - 1)], ws.at[2])
        wait_all(w2.at[pl.ds(0, NP // 2 - 1)], ws.at[3])

    @pl.when(me >= RED)
    def _():
        wait_all(w2.at[pl.ds(0, RED)], ws.at[0])

    for c in outs:
        c.wait()
    last_own().wait()
    with jax.named_scope("waitxy"):
        wait_all(got_o.at[pl.ds(0, NP - 1)], rr.at[7])


def on_device(pooled, cotangent, bilinear, bag_ids, bag_lens, row_home):
    any_ = pl.BlockSpec(memory_space=pl.ANY)
    dma = pltpu.SemaphoreType.DMA
    acc, got, code, w4 = pl.pallas_call(
        body,
        out_shape=(
            jax.ShapeDtypeStruct((256, F * D), F32),
            jax.ShapeDtypeStruct((NP, CAP, D), BF16),
            jax.ShapeDtypeStruct((8, 128), I32),
            jax.ShapeDtypeStruct((RED // 2, 2, 32, D), BF16),
        ),
        in_specs=[any_] * 6,
        out_specs=[any_] * 4,
        scratch_shapes=[
            pltpu.VMEM((ROWS, D), BF16),
            pltpu.VMEM((28, TOK, D), BF16),
            pltpu.VMEM((F - 1, D, D), BF16),
            pltpu.VMEM((F, BAG, TOK), I32),
            pltpu.VMEM((F, TOK), I32),
            pltpu.VMEM((512 * F, 128), I32),
            pltpu.VMEM((F, TOK, D), BF16),
            pltpu.VMEM((F - 1, TOK, D), BF16),
            pltpu.VMEM((F - 1, TOK, D), F32),
            pltpu.VMEM((F - 1, TOK, D), F32),
            pltpu.VMEM(((F - 1) * D, D), BF16),
            pltpu.VMEM((F * BAG, 128), I32),
            pltpu.VMEM((F * BAG, 128), F32),
            pltpu.VMEM((F * BAG, 128), F32),
            pltpu.VMEM((64, 128), I32),
            pltpu.VMEM((NZ, 8, 128), I32),
            pltpu.VMEM((NP, 1, 128), I32),
            pltpu.VMEM((NP, 1, 128), I32),
            pltpu.VMEM((NZ, 8, 128), I32),
            pltpu.VMEM((NZ, ROWS, D), BF16),
            pltpu.VMEM((NZ, NP, CAP, D), BF16),
            pltpu.VMEM((NZ, NP, CAP, D), BF16),
            pltpu.VMEM((256, F * D), F32),
            pltpu.VMEM((NP, 32, D), BF16),
            pltpu.VMEM((NZ, 4, D), F32),
            pltpu.VMEM((RED // 2, 2, 32, D), BF16),
            pltpu.VMEM((NZ, 4, D), F32),
            pltpu.VMEM((NZ, 4, D), F32),
            dma((7,)),
            dma((2, 4, NCH)),
            dma((2, 4, NCH)),
            dma,
            dma((NZ,)),
            dma,
            dma,
            dma((8,)),
            dma((8,)),
            dma((5,)),
            dma((5,)),
        ],
        compiler_params=pltpu.CompilerParams(
            collective_id=0, has_side_effects=True, vmem_limit_bytes=60 * 2**20
        ),
    )(
        pooled.reshape(ROWS, D),
        cotangent.transpose(1, 0, 2),
        bilinear,
        bag_ids.transpose(1, 2, 0),
        bag_lens.transpose(1, 0),
        row_home.reshape(F, 512, 128).transpose(1, 0, 2).reshape(512 * F, 128),
    )
    wg, table = pl.pallas_call(
        finish,
        out_shape=(
            jax.ShapeDtypeStruct(((F - 1) * D, D), F32),
            jax.ShapeDtypeStruct((256 * F, D), F32),
        ),
        in_specs=[any_] * 4,
        out_specs=[any_] * 2,
        scratch_shapes=[
            pltpu.VMEM((256, F * D), F32),
            pltpu.VMEM((NP, CAP, D), BF16),
            pltpu.VMEM((8, 128), I32),
            pltpu.VMEM(((F - 1) * D, D), BF16),
            pltpu.VMEM(((F - 1) * D, D), F32),
            pltpu.VMEM((256, F * D), F32),
            pltpu.VMEM((256 * F, D), F32),
            dma((6,)),
        ],
        compiler_params=pltpu.CompilerParams(vmem_limit_bytes=60 * 2**20),
    )(acc, got, code, w4.reshape((F - 1) * D, D))
    return wg.reshape(F - 1, D, D), table.reshape(256, F, D)


def solution(mesh):
    placed = (
        P(("gx", "gy"), None, None),
        P(("gx", "gy"), None, None),
        P(),
        P(("gx", "gy"), None, None),
        P(("gx", "gy"), None),
        P(),
    )
    return jax.shard_map(
        on_device,
        mesh=mesh,
        in_specs=placed,
        out_specs=(P(), P(("gx", "gy"), None, None)),
        check_vma=False,
    )
```

```python
import functools

import jax
import jax.numpy as jnp
from jax import lax
from jax.experimental import pallas as pl
from jax.experimental.pallas import tpu as pltpu
from jax.sharding import PartitionSpec as P

MESH = pl.DeviceIdType.MESH
F = 8
BAG = 4
D = 128
TOK = 128
CAP = 32
NZ = 8
NP = 32
ROWS = F * TOK
NCH = 4
RED = 28
PAIR = {(i, j): p for p, (i, j) in enumerate((i, j) for i in range(F) for j in range(i + 1, F))}
STEPS = ((2, 2), (1, 2), (2, 1), (3, 2), (2, 3), (1, 1), (3, 3), (2, 0), (0, 2), (1, 3), (3, 1), (1, 0), (0, 1), (3, 0), (0, 3))
F32, BF16, I32, I16 = jnp.float32, jnp.bfloat16, jnp.int32, jnp.int16


def dev(z, p):
    return (2 * z + p // 16, p % 16)


def iota(shape, dim):
    return lax.broadcasted_iota(I32, shape, dim)


def bf(x):
    return x.astype(F32).astype(BF16)


def onehot(mask):
    return jnp.where(mask, jnp.ones((), BF16), jnp.zeros((), BF16))


def only(mask, x):
    return jnp.where(mask, x, jnp.zeros((), BF16))


def colsum(x):
    acc = x[:16]
    for i in range(16, x.shape[0], 16):
        acc = acc + x[i : i + 16]
    return jnp.sum(acc.astype(F32), axis=0, keepdims=True)


def dot(a, b, ca=1, cb=0):
    return lax.dot_general(a, b, (((ca,), (cb,)), ((), ())), preferred_element_type=F32)


def wait_all(ref, sem):
    pltpu.make_async_copy(ref, ref, sem).wait()


def add_slots(code, rows, acc):
    field, local = (code & 15).astype(F32), bf(code >> 4)
    q_iota = bf(iota((256, 128), 0))
    lhs, rhs = [], []
    for g in range(8):
        fcol = jnp.broadcast_to(field[g : g + 1, :], (128, 128)).T.astype(BF16)
        v = rows[pl.ds(g * 4, 4)].reshape(128, D)
        rhs.append(jnp.concatenate([only(fcol == jnp.asarray(f + 1, BF16), v) for f in range(F)], axis=1))
        lhs.append(onehot(q_iota == local[g : g + 1, :]))
        if g % 4 == 3:
            acc[...] += dot(jnp.concatenate(lhs, axis=1), jnp.concatenate(rhs, axis=0))
            lhs, rhs = [], []


def finish(acc_h, got_h, code_h, w4_h, wg_o, tab_o, acc, got, code, w4, wg, part, table, sem):
    loads = [pltpu.make_async_copy(a, b, sem.at[n]) for n, (a, b) in enumerate([(got_h, got), (code_h, code), (w4_h, w4), (acc_h, acc)])]
    for c in loads:
        c.start()
    part[...] = jnp.zeros_like(part)
    loads[0].wait()
    loads[1].wait()
    add_slots(code[...], got, part)
    loads[2].wait()
    wg[...] = w4[...].astype(F32).reshape((F - 1) * D, D)
    wg_out = pltpu.make_async_copy(wg, wg_o, sem.at[4])
    wg_out.start()
    loads[3].wait()
    for f in range(F):
        cols = slice(f * D, f * D + D)
        table[pl.ds(f, 256, stride=F), :] = acc[:, cols] + part[:, cols]
    table_out = pltpu.make_async_copy(table, tab_o, sem.at[5])
    table_out.start()
    wg_out.wait()
    table_out.wait()


def body(
    pool_h, cot_h, bil_h, ids_h, lens_h, home_h,
    acc_o, got_o, code_o, w4_o,
    pool, cot, bil, ids, lens, home,
    pf, up, proj, back, share,
    own, loc, live, m4, mall, dsend, drecv, cbuf,
    vbuf, stage, got,
    acc, w2, w3, w4, part,
    lsem, zs, zr, ms, mr, ds_, dr, ss, rr, ws, wr,
):
    gx, gy = lax.axis_index("gx"), lax.axis_index("gy")
    z, me = gx // 2, (gx % 2) * 16 + gy
    core = gy % 2

    loads = [
        pltpu.make_async_copy(a, b, lsem.at[n])
        for n, (a, b) in enumerate(
            [(pool_h, pool), (bil_h, bil), (cot_h, cot), (ids_h, ids), (lens_h, lens), (home_h, home)]
        )
    ]
    for c in loads:
        c.start()

    bar = pltpu.get_barrier_semaphore()

    for t in (4, 3, 5, 2, 6, 1, 7):
        pl.semaphore_signal(bar, inc=1, device_id=dev((z + t) % NZ, me), device_id_type=MESH)
    for j in range(NP - 1, 0, -1):
        pl.semaphore_signal(bar, inc=1, device_id=dev(z, me ^ j), device_id_type=MESH)

    with jax.named_scope("perm"):
        loads[0].wait()
        perm = jnp.where(iota((128, 128), 1) == (iota((128, 128), 0) % 16) * F + iota((128, 128), 0) // 16, 1.0, 0.0).astype(BF16)
        x = jnp.concatenate([pool[pl.ds(g * 128, 128), :] for g in range(8)], axis=1)
        y = dot(perm, x).astype(BF16)
        for g in range(8):
            for f in range(F):
                pf[f, pl.ds(g * 16, 16), :] = y[f * 16 : f * 16 + 16, g * 128 : g * 128 + 128]
    with jax.named_scope("grads"):
        loads[1].wait()
        loads[2].wait()
        for i in range(F - 1):
            proj[i] = dot(pf[i], bil[i])
        for r in range(0, TOK, 16):
            rows = pl.ds(r, 16)
            pj = [pf[j, rows, :].astype(F32) for j in range(F)]
            for i in range(F - 1):
                run = cot[PAIR[i, i + 1], rows, :].astype(F32) * pj[i + 1]
                for j in range(i + 2, F):
                    run = run + cot[PAIR[i, j], rows, :].astype(F32) * pj[j]
                up[i, rows, :] = run.astype(BF16)
        for i in range(F - 1):
            back[i] = dot(up[i], bil[i], 1, 1)
        for r in range(0, TOK, 16):
            rows = pl.ds(r, 16)
            for i in range(F):
                run = back[i, rows, :] if i < F - 1 else cot[PAIR[0, i], rows, :].astype(F32) * proj[0, rows, :]
                for k in range(0 if i < F - 1 else 1, i):
                    run = run + cot[PAIR[k, i], rows, :].astype(F32) * proj[k, rows, :]
                vbuf[0, pl.ds(i * TOK + r, 16), :] = run.astype(BF16)
        for i in range(F - 1):
            share[pl.ds(i * D, D), :] = dot(pf[i], up[i], 0, 0).astype(BF16)

    with jax.named_scope("barrier"):
        pl.semaphore_wait(bar, NP - 1 + NZ - 1)

    piece = ROWS // NCH

    def zcopy(e, t, c):
        src = jnp.where(t == 1, 0, 2 * t - 3 + e)
        dst = jnp.where(t == 4, 7, 2 * t - 1 + e)
        at = jnp.where(e == 0, c, NCH - 1 - c)
        rows = pl.ds(pl.multiple_of(at * piece, piece), piece)
        to = (z + jnp.where(e == core, 1, NZ - 1)) % NZ
        return pltpu.make_async_remote_copy(
            vbuf.at[src, rows], vbuf.at[dst, rows], zs.at[e, t - 1, c], zr.at[e, t - 1, c],
            device_id=dev(to, me), device_id_type=MESH,
        )

    def first_hop(e):
        for c in range(NCH):
            zcopy(e, 1, c).start()

    first_hop(0)

    def w2copy(r):
        return pltpu.make_async_remote_copy(
            share.at[pl.ds(pl.multiple_of(r * 32, 32), 32)], w2.at[me], ws.at[0], wr.at[0],
            device_id=dev(z, r), device_id_type=MESH,
        )

    def shares_out():
        @pl.loop(0, NP)
        def _(j):
            r = me ^ j

            @pl.when((r < RED) & (j > 0))
            def _():
                w2copy(r).start()

    with jax.named_scope("shares_out"):
        shares_out()

    @pl.when(gx >= 0)
    def _():
        with jax.named_scope("lookup"):
            loads[3].wait()
            loads[4].wait()
            loads[5].wait()
            hi_iota, lo_iota = iota((512, 128), 0).astype(I16), bf(iota((128, 128), 0))
            for f in range(F):
                t = home[pl.ds(f, 512, stride=F), :].T
                table = bf(jnp.concatenate([t >> 8, t & 255], axis=0))
                hi, lo = (ids[f] >> 7).astype(I16), bf(ids[f] & 127)
                oh = jnp.concatenate([onehot(hi_iota == hi[k : k + 1]) for k in range(BAG)], axis=1)
                out = dot(table, oh).astype(BF16)
                for k in range(BAG):
                    mask = lo_iota == lo[k : k + 1]
                    cols = slice(k * 128, k * 128 + 128)
                    row = f * BAG + k
                    own[row : row + 1, :] = colsum(only(mask, out[:128, cols])).astype(I32)
                    loc[row : row + 1, :] = colsum(only(mask, out[128:, cols]))
                    live[row : row + 1, :] = jnp.where(lens[f : f + 1, :] > k, float(f + 1), 0.0)

    first_hop(1)

    @pl.when(gx >= 0)
    def _():
        with jax.named_scope("rank"):
            tri = jnp.where(iota((256, 256), 0) <= iota((256, 256), 1), 1.0, 0.0).astype(BF16)
            own_iota, o4_iota, rr_iota = bf(iota((256, 128), 0)), bf(iota((64, 128), 0)), bf(iota((128, 128), 0))
            lane = bf(iota((1, 128), 1) + 1)
            o = own[...]
            o_b, o4_b, oc_b = bf(o), bf(o >> 2), bf((o & 3) * CAP - 1)
            loc_b, live_b = loc[...].astype(BF16), live[...].astype(BF16)
            before = jnp.zeros((256, 128), BF16)
            lhs, rhs = [], []
            for j in range(16):
                hit = [own_iota == o_b[r : r + 1] for r in (2 * j, 2 * j + 1)]
                count = dot(jnp.concatenate([onehot(h) for h in hit], axis=1), tri).astype(BF16)
                for n in range(2):
                    r = slice(2 * j + n, 2 * j + n + 1)
                    rank = colsum(only(hit[n], count[:, n * 128 : n * 128 + 128] + before))
                    spot = rr_iota == oc_b[r] + rank.astype(BF16)
                    four = o4_iota == o4_b[r]
                    lhs.append(jnp.concatenate([only(spot, lane), only(spot, loc_b[r])], axis=0))
                    rhs.append(jnp.concatenate([onehot(four), only(four, live_b[r])], axis=0))
                before = before + jnp.broadcast_to(count[:, 255:], (256, 128))
            table = dot(jnp.concatenate(lhs, axis=1), jnp.concatenate(rhs, axis=1), 1, 1).T
            b1 = table[:64, :128]
            f1 = jnp.round(table[64:, :128] / jnp.maximum(b1, 1.0))
            m4[...] = jnp.where(b1 > 0, (b1 - 1.0) + 128.0 * f1 + 2048.0 * table[:64, 128:], 0.0).astype(I32)
    mall[0] = m4[pl.ds(pl.multiple_of(z * 8, 8), 8), :]

    def mcopy(n):
        t = (n + 1) // 2
        to = (z + jnp.where((n - 1) % 2 == core, t, NZ - t)) % NZ
        return pltpu.make_async_remote_copy(
            m4.at[pl.ds(pl.multiple_of(to * 8, 8), 8)], mall.at[n], ms, mr.at[n], device_id=dev(to, me), device_id_type=MESH
        )

    @pl.loop(1, NZ)
    def _(t):
        mcopy(t).start()


    lane128 = iota((128, 128), 1).astype(I16)

    def gather(idx):
        for pq in range(8):
            row = mall[idx, pl.ds(pq, 1), :] & 2047
            col = jnp.broadcast_to(row, (128, 128)).T.astype(I16)
            g = jnp.concatenate([onehot(col == lane128 + jnp.asarray(128 * (f + 1), I16)) for f in range(F)], axis=1)
            rows = dot(g, vbuf[idx]).astype(BF16)
            stage[idx, pl.ds(pq * 4, 4)] = rows.reshape(4, CAP, D)

    def xycopy(idx, q):
        return pltpu.make_async_remote_copy(
            stage.at[idx, q], got.at[idx, me], ss.at[idx], rr.at[idx], device_id=dev(z, q), device_id_type=MESH
        )

    way = 1 + 2 * core
    at_x, at_y = (me // 2 % 2) * 2 + me // 16, me // 4 % 4

    def chip(dx, dy, c):
        x, y = (at_x + way * dx) % 4, (at_y + way * dy) % 4
        return (x % 2) * 16 + y * 4 + (x // 2) * 2 + c

    others = [chip(dx, dy, c) for dx, dy in STEPS for c in range(2)] + [me ^ 1]

    def send(idx):
        got[idx, me] = stage[idx, me]
        for q in others:
            xycopy(idx, q).start()

    def last_own():
        return pltpu.make_async_copy(stage.at[7, me], got_o.at[me], lsem.at[6])

    def send_last():
        last_own().start()
        for q in others:
            pltpu.make_async_remote_copy(
                stage.at[7, q], got_o.at[me], ss.at[7], rr.at[7], device_id=dev(z, q), device_id_type=MESH
            ).start()

    def accumulate(idx):
        with jax.named_scope("waitxy"):
            wait_all(got.at[idx, pl.ds(0, NP - 1)], rr.at[idx])
        add_slots(cbuf[idx], got.at[idx], acc)

    def fold(y):
        y = y + pltpu.roll(y, 7, 0)
        return y + pltpu.roll(y, 6, 0)

    def dcopy(q):
        return pltpu.make_async_remote_copy(
            dsend.at[q], drecv.at[me], ds_, dr, device_id=dev(z, q), device_id_type=MESH
        )

    def targets_out(quads):
        row4, block = iota((8, 128), 0) % 4, iota((8, 128), 1) // CAP
        for pq in quads:
            x = mall[:, pq, :] >> 7
            turned = [pltpu.roll(x, s * CAP, 1) if s else x for s in range(4)]
            for j in range(4):
                y = sum(jnp.where((block == row4) & ((row4 + 4 - j) % 4 == s), turned[s], 0) for s in range(4))
                y = fold(y)
                dsend[pq * 4 + j] = y[0:1] + (y[4:5] << 16)

    def targets_first():
        for n in range(3, NZ):
            mcopy(n).wait_recv()
        targets_out(range(4))

    def targets_rest():
        targets_out(range(4, 8))
        drecv[me] = dsend[me]

        @pl.loop(1, NP)
        def _(j):
            dcopy(me ^ j).start()

    def targets_in():
        many = drecv.at[pl.ds(0, NP - 1)]
        pltpu.make_async_copy(many, many, dr).wait()
        row4, block = iota((8, 128), 0) % 4, iota((8, 128), 1) // CAP
        for v in range(4):
            words = drecv[pl.ds(v * 8, 8)].reshape(8, 128)
            for r in range(2):
                x = (words >> 16) if r else (words & 0xFFFF)
                turned = [pltpu.roll(x, s * CAP, 1) if s else x for s in range(4)]
                for m in range(4):
                    y = sum(jnp.where((block == row4) & ((row4 + 4 - m) % 4 == s), turned[s], 0) for s in range(4))
                    y = fold(y)
                    for h in range(2):
                        cbuf[4 * r + m, 2 * v + h : 2 * v + h + 1, :] = y[4 * h : 4 * h + 1]

    def w3copy(t):
        to = (z + t) % NZ
        return pltpu.make_async_remote_copy(
            part.at[to], w3.at[z], ws.at[1], wr.at[1], device_id=dev(to, me), device_id_type=MESH
        )

    def rows_copy(q):
        mine = w4.at[me // 2, core, z]
        return pltpu.make_async_remote_copy(
            mine, mine, ws.at[2], wr.at[2], device_id=dev(z, q), device_id_type=MESH
        )

    def column_copy(t):
        mine = w4.at[:, core, z]
        return pltpu.make_async_remote_copy(
            mine, mine, ws.at[3], wr.at[3], device_id=dev((z + t) % NZ, me), device_id_type=MESH
        )

    def w4side():
        return pltpu.make_async_remote_copy(
            w4.at[:, core], w4_o.at[:, core], ws.at[4], wr.at[4], device_id=dev(z, me ^ 1), device_id_type=MESH
        )

    def w4own():
        return pltpu.make_async_copy(w4.at[:, core], w4_o.at[:, core], lsem.at[2])

    adder = me < RED

    def weight_add():
        @pl.when(adder)
        def _():
            w2[me] = share[pl.ds(pl.multiple_of(me * 32, 32), 32), :]
            wait_all(w2.at[pl.ds(0, NP - 1)], wr.at[0])
            total = w2[0].astype(F32)
            for i in range(1, NP):
                total = total + w2[i].astype(F32)
            part[...] = total.reshape(NZ, 4, D)
            w3[z] = part[z]

            @pl.loop(1, NZ)
            def _(t):
                w3copy(t).start()

    def weight_column():
        @pl.when(adder)
        def _():
            wait_all(w3.at[pl.ds(0, NZ - 1)], wr.at[1])
            total = w3[0]
            for i in range(1, NZ):
                total = total + w3[i]
            w4[me // 2, core, z] = total.astype(BF16)

            @pl.loop(1, NP // 2)
            def _(j):
                rows_copy(me ^ (2 * j)).start()

    def weight_spread():
        @pl.when(adder)
        def _():
            wait_all(w4.at[pl.ds(0, RED // 2 - 1), 0, 0], wr.at[2])

        @pl.when(me >= RED)
        def _():
            wait_all(w4.at[:, 0, 0], wr.at[2])

        @pl.loop(1, NZ)
        def _(t):
            column_copy(t).start()

    def weight_side():
        wait_all(w4.at[:, 0, pl.ds(0, NZ - 1)], wr.at[3])
        w4side().start()
        w4own().start()

    acc[...] = jnp.zeros_like(acc)

    def pass_on(n, c):
        e, t = (n - 1) % 2, (n + 1) // 2
        with jax.named_scope(f"waitz{c}"):
            zcopy(e, t, c).wait_recv()

        @pl.when((t < 3) | (c < NCH // 2))
        def _():
            zcopy(e, t + 1, c).start()

    @pl.loop(0, 9)
    def _(n):
        @pl.when((n > 0) & (n < 7))
        def _():
            pass_on(n, 2)

            @pl.when((n > 1) & (n < 6))
            def _():
                pass_on(n + 1, 0)

            pass_on(n, 3)

        @pl.when(n == 7)
        def _():
            with jax.named_scope("waitz4"):
                for c in range(NCH // 2):
                    for e in range(2):
                        zcopy(e, 4, c).wait_recv()

        @pl.when(n < 8)
        def _():
            @pl.when((n == 1) | (n == 2))
            def _():
                with jax.named_scope("waitm"):
                    mcopy(n).wait_recv()

            with jax.named_scope("gather"):
                gather(n)

            @pl.when(n < 7)
            def _():
                with jax.named_scope("send"):
                    send(n)

            @pl.when(n == 7)
            def _():
                with jax.named_scope("send"):
                    send_last()


        def once(when, what):
            @pl.when(n == when)
            def _():
                with jax.named_scope(what.__name__):
                    what()

        def add(lo, hi):
            @pl.loop(lo, hi)
            def _(m):
                with jax.named_scope("acc"):
                    accumulate(m)

        @pl.when(n < 2)
        def _():
            pass_on(n + 1, 0)

        @pl.when(n < 6)
        def _():
            pass_on(n + 1, 1)

        once(1, weight_add)
        once(2, targets_first)
        once(3, targets_rest)
        once(4, weight_column)
        once(6, targets_in)
        once(7, weight_spread)
        add(jnp.where(n == 8, 1, 0), jnp.where(n == 8, 7, jnp.where(n == 6, 1, 0)))
        once(8, weight_side)

    outs = [pltpu.make_async_copy(acc, acc_o, lsem.at[0]), pltpu.make_async_copy(cbuf.at[7], code_o, lsem.at[1])]
    for c in outs:
        c.start()
    for t in range(1, 5):
        for d in range(2):
            for c in range(NCH):
                if t < 4 or c < NCH // 2:
                    zcopy(d, t, c).wait_send()
    wait_all(mall.at[pl.ds(0, NZ - 1)], ms)
    wait_all(dsend.at[pl.ds(0, NP - 1)], ds_)
    wait_all(w4.at[:, 0, pl.ds(0, NZ - 1)], ws.at[3])
    for k in range(8):
        wait_all(stage.at[k, pl.ds(0, NP - 1)], ss.at[k])

    @pl.when(adder)
    def _():
        wait_all(w2.at[pl.ds(0, RED - 1)], ws.at[0])
        wait_all(w3.at[pl.ds(0, NZ - 1)], ws.at[1])
        wait_all(w4.at[pl.ds(0, 5), 0, pl.ds(0, 3)], ws.at[2])

    @pl.when(me >= RED)
    def _():
        wait_all(w2.at[pl.ds(0, RED)], ws.at[0])

    for c in outs:
        c.wait()
    last_own().wait()
    with jax.named_scope("waitside"):
        w4own().wait()
        w4side().wait()
    with jax.named_scope("waitxy"):
        wait_all(got_o.at[pl.ds(0, NP - 1)], rr.at[7])


def on_device(pooled, cotangent, bilinear, bag_ids, bag_lens, row_home):
    any_ = pl.BlockSpec(memory_space=pl.ANY)
    dma = pltpu.SemaphoreType.DMA
    acc, got, code, w4 = pl.pallas_call(
        body,
        out_shape=(
            jax.ShapeDtypeStruct((256, F * D), F32),
            jax.ShapeDtypeStruct((NP, CAP, D), BF16),
            jax.ShapeDtypeStruct((8, 128), I32),
            jax.ShapeDtypeStruct((RED // 2, 2, NZ, 4, D), BF16),
        ),
        in_specs=[any_] * 6,
        out_specs=[any_] * 4,
        scratch_shapes=[
            pltpu.VMEM((ROWS, D), BF16),
            pltpu.VMEM((28, TOK, D), BF16),
            pltpu.VMEM((F - 1, D, D), BF16),
            pltpu.VMEM((F, BAG, TOK), I32),
            pltpu.VMEM((F, TOK), I32),
            pltpu.VMEM((512 * F, 128), I32),
            pltpu.VMEM((F, TOK, D), BF16),
            pltpu.VMEM((F - 1, TOK, D), BF16),
            pltpu.VMEM((F - 1, TOK, D), F32),
            pltpu.VMEM((F - 1, TOK, D), F32),
            pltpu.VMEM(((F - 1) * D, D), BF16),
            pltpu.VMEM((F * BAG, 128), I32),
            pltpu.VMEM((F * BAG, 128), F32),
            pltpu.VMEM((F * BAG, 128), F32),
            pltpu.VMEM((64, 128), I32),
            pltpu.VMEM((NZ, 8, 128), I32),
            pltpu.VMEM((NP, 1, 128), I32),
            pltpu.VMEM((NP, 1, 128), I32),
            pltpu.VMEM((NZ, 8, 128), I32),
            pltpu.VMEM((NZ, ROWS, D), BF16),
            pltpu.VMEM((NZ, NP, CAP, D), BF16),
            pltpu.VMEM((NZ, NP, CAP, D), BF16),
            pltpu.VMEM((256, F * D), F32),
            pltpu.VMEM((NP, 32, D), BF16),
            pltpu.VMEM((NZ, 4, D), F32),
            pltpu.VMEM((RED // 2, 2, NZ, 4, D), BF16),
            pltpu.VMEM((NZ, 4, D), F32),
            dma((7,)),
            dma((2, 4, NCH)),
            dma((2, 4, NCH)),
            dma,
            dma((NZ,)),
            dma,
            dma,
            dma((8,)),
            dma((8,)),
            dma((5,)),
            dma((5,)),
        ],
        compiler_params=pltpu.CompilerParams(
            collective_id=0, has_side_effects=True, vmem_limit_bytes=60 * 2**20
        ),
    )(
        pooled.reshape(ROWS, D),
        cotangent.transpose(1, 0, 2),
        bilinear,
        bag_ids.transpose(1, 2, 0),
        bag_lens.transpose(1, 0),
        row_home.reshape(F, 512, 128).transpose(1, 0, 2).reshape(512 * F, 128),
    )
    wg, table = pl.pallas_call(
        finish,
        out_shape=(
            jax.ShapeDtypeStruct(((F - 1) * D, D), F32),
            jax.ShapeDtypeStruct((256 * F, D), F32),
        ),
        in_specs=[any_] * 4,
        out_specs=[any_] * 2,
        scratch_shapes=[
            pltpu.VMEM((256, F * D), F32),
            pltpu.VMEM((NP, CAP, D), BF16),
            pltpu.VMEM((8, 128), I32),
            pltpu.VMEM(((F - 1) * D // 4, 4, D), BF16),
            pltpu.VMEM(((F - 1) * D, D), F32),
            pltpu.VMEM((256, F * D), F32),
            pltpu.VMEM((256 * F, D), F32),
            dma((6,)),
        ],
        compiler_params=pltpu.CompilerParams(vmem_limit_bytes=60 * 2**20),
    )(acc, got, code, w4.reshape((F - 1) * D // 4, 4, D))
    return wg.reshape(F - 1, D, D), table.reshape(256, F, D)


def solution(mesh):
    placed = (
        P(("gx", "gy"), None, None),
        P(("gx", "gy"), None, None),
        P(),
        P(("gx", "gy"), None, None),
        P(("gx", "gy"), None),
        P(),
    )
    return jax.shard_map(
        on_device,
        mesh=mesh,
        in_specs=placed,
        out_specs=(P(), P(("gx", "gy"), None, None)),
        check_vma=False,
    )
```

```python
import functools

import jax
import jax.numpy as jnp
from jax import lax
from jax.experimental import pallas as pl
from jax.experimental.pallas import tpu as pltpu
from jax.sharding import PartitionSpec as P

MESH = pl.DeviceIdType.MESH
F = 8
BAG = 4
D = 128
TOK = 128
CAP = 32
NZ = 8
NP = 32
ROWS = F * TOK
NCH = 4
RED = 28
PAIR = {(i, j): p for p, (i, j) in enumerate((i, j) for i in range(F) for j in range(i + 1, F))}
STEPS = ((2, 2), (1, 2), (2, 1), (3, 2), (2, 3), (1, 1), (3, 3), (2, 0), (0, 2), (1, 3), (3, 1), (1, 0), (0, 1), (3, 0), (0, 3))
F32, BF16, I32, I16 = jnp.float32, jnp.bfloat16, jnp.int32, jnp.int16


def dev(z, p):
    return (2 * z + p // 16, p % 16)


def iota(shape, dim):
    return lax.broadcasted_iota(I32, shape, dim)


def bf(x):
    return x.astype(F32).astype(BF16)


def onehot(mask):
    return jnp.where(mask, jnp.ones((), BF16), jnp.zeros((), BF16))


def only(mask, x):
    return jnp.where(mask, x, jnp.zeros((), BF16))


def colsum(x):
    acc = x[:16]
    for i in range(16, x.shape[0], 16):
        acc = acc + x[i : i + 16]
    return jnp.sum(acc.astype(F32), axis=0, keepdims=True)


def dot(a, b, ca=1, cb=0):
    return lax.dot_general(a, b, (((ca,), (cb,)), ((), ())), preferred_element_type=F32)


def wait_all(ref, sem):
    pltpu.make_async_copy(ref, ref, sem).wait()


def add_slots(code, rows, acc):
    field, local = (code & 15).astype(F32), bf(code >> 4)
    q_iota = bf(iota((256, 128), 0))
    lhs, rhs = [], []
    for g in range(8):
        fcol = jnp.broadcast_to(field[g : g + 1, :], (128, 128)).T.astype(BF16)
        v = rows[pl.ds(g * 4, 4)].reshape(128, D)
        rhs.append(jnp.concatenate([only(fcol == jnp.asarray(f + 1, BF16), v) for f in range(F)], axis=1))
        lhs.append(onehot(q_iota == local[g : g + 1, :]))
        if g % 4 == 3:
            acc[...] += dot(jnp.concatenate(lhs, axis=1), jnp.concatenate(rhs, axis=0))
            lhs, rhs = [], []


def finish(acc_h, got_h, code_h, w4_h, wg_o, tab_o, acc, got, code, w4, wg, part, table, sem):
    loads = [pltpu.make_async_copy(a, b, sem.at[n]) for n, (a, b) in enumerate([(got_h, got), (code_h, code), (w4_h, w4), (acc_h, acc)])]
    for c in loads:
        c.start()
    part[...] = jnp.zeros_like(part)
    loads[0].wait()
    loads[1].wait()
    add_slots(code[...], got, part)
    loads[2].wait()
    wg[...] = w4[...].astype(F32).reshape((F - 1) * D, D)
    wg_out = pltpu.make_async_copy(wg, wg_o, sem.at[4])
    wg_out.start()
    loads[3].wait()
    for f in range(F):
        cols = slice(f * D, f * D + D)
        table[pl.ds(f, 256, stride=F), :] = acc[:, cols] + part[:, cols]
    table_out = pltpu.make_async_copy(table, tab_o, sem.at[5])
    table_out.start()
    wg_out.wait()
    table_out.wait()


def body(
    pool_h, cot_h, bil_h, ids_h, lens_h, home_h,
    acc_o, got_o, code_o, w4_o,
    pool, cot, bil, ids, lens, home,
    pf, up, proj, back, share,
    own, loc, live, m4, mall, dsend, drecv, cbuf,
    vbuf, stage, got,
    acc, w2, w3, w4, part,
    lsem, zs, zr, ms, mr, ds_, dr, ss, rr, ws, wr,
):
    gx, gy = lax.axis_index("gx"), lax.axis_index("gy")
    z, me = gx // 2, (gx % 2) * 16 + gy
    core = gy % 2

    loads = [
        pltpu.make_async_copy(a, b, lsem.at[n])
        for n, (a, b) in enumerate(
            [(pool_h, pool), (bil_h, bil), (cot_h, cot), (ids_h, ids), (lens_h, lens), (home_h, home)]
        )
    ]
    for c in loads:
        c.start()

    bar = pltpu.get_barrier_semaphore()

    for t in (4, 3, 5, 2, 6, 1, 7):
        pl.semaphore_signal(bar, inc=1, device_id=dev((z + t) % NZ, me), device_id_type=MESH)
    for j in range(NP - 1, 0, -1):
        pl.semaphore_signal(bar, inc=1, device_id=dev(z, me ^ j), device_id_type=MESH)

    with jax.named_scope("perm"):
        loads[0].wait()
        perm = jnp.where(iota((128, 128), 1) == (iota((128, 128), 0) % 16) * F + iota((128, 128), 0) // 16, 1.0, 0.0).astype(BF16)
        x = jnp.concatenate([pool[pl.ds(g * 128, 128), :] for g in range(8)], axis=1)
        y = dot(perm, x).astype(BF16)
        for g in range(8):
            for f in range(F):
                pf[f, pl.ds(g * 16, 16), :] = y[f * 16 : f * 16 + 16, g * 128 : g * 128 + 128]
    with jax.named_scope("grads"):
        loads[1].wait()
        loads[2].wait()
        for i in range(F - 1):
            proj[i] = dot(pf[i], bil[i])
        for r in range(0, TOK, 16):
            rows = pl.ds(r, 16)
            pj = [pf[j, rows, :].astype(F32) for j in range(F)]
            for i in range(F - 1):
                run = cot[PAIR[i, i + 1], rows, :].astype(F32) * pj[i + 1]
                for j in range(i + 2, F):
                    run = run + cot[PAIR[i, j], rows, :].astype(F32) * pj[j]
                up[i, rows, :] = run.astype(BF16)
        for i in range(F - 1):
            back[i] = dot(up[i], bil[i], 1, 1)
        for r in range(0, TOK, 16):
            rows = pl.ds(r, 16)
            for i in range(F):
                run = back[i, rows, :] if i < F - 1 else cot[PAIR[0, i], rows, :].astype(F32) * proj[0, rows, :]
                for k in range(0 if i < F - 1 else 1, i):
                    run = run + cot[PAIR[k, i], rows, :].astype(F32) * proj[k, rows, :]
                vbuf[0, pl.ds(i * TOK + r, 16), :] = run.astype(BF16)
        for i in range(F - 1):
            share[pl.ds(i * D, D), :] = dot(pf[i], up[i], 0, 0).astype(BF16)

    with jax.named_scope("barrier"):
        pl.semaphore_wait(bar, NP - 1 + NZ - 1)

    piece = ROWS // NCH

    def zcopy(e, t, c):
        src = jnp.where(t == 1, 0, 2 * t - 3 + e)
        dst = jnp.where(t == 4, 7, 2 * t - 1 + e)
        at = jnp.where(e == 0, c, NCH - 1 - c)
        rows = pl.ds(pl.multiple_of(at * piece, piece), piece)
        to = (z + jnp.where(e == core, 1, NZ - 1)) % NZ
        return pltpu.make_async_remote_copy(
            vbuf.at[src, rows], vbuf.at[dst, rows], zs.at[e, t - 1, c], zr.at[e, t - 1, c],
            device_id=dev(to, me), device_id_type=MESH,
        )

    def first_hop(e):
        for c in range(NCH):
            zcopy(e, 1, c).start()

    first_hop(0)

    def w2copy(r):
        return pltpu.make_async_remote_copy(
            share.at[pl.ds(pl.multiple_of(r * 32, 32), 32)], w2.at[me], ws.at[0], wr.at[0],
            device_id=dev(z, r), device_id_type=MESH,
        )

    def shares_out():
        for j in range(1, NP):
            r = me ^ j

            @pl.when(r < RED)
            def _():
                w2copy(r).start()

    with jax.named_scope("shares_out"):
        shares_out()

    @pl.when(gx >= 0)
    def _():
        with jax.named_scope("lookup"):
            loads[3].wait()
            loads[4].wait()
            loads[5].wait()
            hi_iota, lo_iota = iota((512, 128), 0).astype(I16), bf(iota((128, 128), 0))
            for f in range(F):
                t = home[pl.ds(f, 512, stride=F), :].T
                table = bf(jnp.concatenate([t >> 8, t & 255], axis=0))
                hi, lo = (ids[f] >> 7).astype(I16), bf(ids[f] & 127)
                oh = jnp.concatenate([onehot(hi_iota == hi[k : k + 1]) for k in range(BAG)], axis=1)
                out = dot(table, oh).astype(BF16)
                for k in range(BAG):
                    mask = lo_iota == lo[k : k + 1]
                    cols = slice(k * 128, k * 128 + 128)
                    row = f * BAG + k
                    own[row : row + 1, :] = colsum(only(mask, out[:128, cols])).astype(I32)
                    loc[row : row + 1, :] = colsum(only(mask, out[128:, cols]))
                    live[row : row + 1, :] = jnp.where(lens[f : f + 1, :] > k, float(f + 1), 0.0)

    first_hop(1)

    @pl.when(gx >= 0)
    def _():
        with jax.named_scope("rank"):
            tri = jnp.where(iota((256, 256), 0) <= iota((256, 256), 1), 1.0, 0.0).astype(BF16)
            own_iota, o4_iota, rr_iota = bf(iota((256, 128), 0)), bf(iota((64, 128), 0)), bf(iota((128, 128), 0))
            lane = bf(iota((1, 128), 1) + 1)
            o = own[...]
            o_b, o4_b, oc_b = bf(o), bf(o >> 2), bf((o & 3) * CAP - 1)
            loc_b, live_b = loc[...].astype(BF16), live[...].astype(BF16)
            before = jnp.zeros((256, 128), BF16)
            lhs, rhs = [], []
            for j in range(16):
                hit = [own_iota == o_b[r : r + 1] for r in (2 * j, 2 * j + 1)]
                count = dot(jnp.concatenate([onehot(h) for h in hit], axis=1), tri).astype(BF16)
                for n in range(2):
                    r = slice(2 * j + n, 2 * j + n + 1)
                    rank = colsum(only(hit[n], count[:, n * 128 : n * 128 + 128] + before))
                    spot = rr_iota == oc_b[r] + rank.astype(BF16)
                    four = o4_iota == o4_b[r]
                    lhs.append(jnp.concatenate([only(spot, lane), only(spot, loc_b[r])], axis=0))
                    rhs.append(jnp.concatenate([onehot(four), only(four, live_b[r])], axis=0))
                before = before + jnp.broadcast_to(count[:, 255:], (256, 128))
            table = dot(jnp.concatenate(lhs, axis=1), jnp.concatenate(rhs, axis=1), 1, 1).T
            b1 = table[:64, :128]
            f1 = jnp.round(table[64:, :128] / jnp.maximum(b1, 1.0))
            m4[...] = jnp.where(b1 > 0, (b1 - 1.0) + 128.0 * f1 + 2048.0 * table[:64, 128:], 0.0).astype(I32)
    mall[0] = m4[pl.ds(pl.multiple_of(z * 8, 8), 8), :]

    def mcopy(n):
        t = (n + 1) // 2
        to = (z + jnp.where((n - 1) % 2 == core, t, NZ - t)) % NZ
        return pltpu.make_async_remote_copy(
            m4.at[pl.ds(pl.multiple_of(to * 8, 8), 8)], mall.at[n], ms, mr.at[n], device_id=dev(to, me), device_id_type=MESH
        )

    @pl.loop(1, NZ)
    def _(t):
        mcopy(t).start()


    lane128 = iota((128, 128), 1).astype(I16)

    def gather(idx):
        for pq in range(8):
            row = mall[idx, pl.ds(pq, 1), :] & 2047
            col = jnp.broadcast_to(row, (128, 128)).T.astype(I16)
            g = jnp.concatenate([onehot(col == lane128 + jnp.asarray(128 * (f + 1), I16)) for f in range(F)], axis=1)
            rows = dot(g, vbuf[idx]).astype(BF16)
            stage[idx, pl.ds(pq * 4, 4)] = rows.reshape(4, CAP, D)

    def xycopy(idx, q):
        return pltpu.make_async_remote_copy(
            stage.at[idx, q], got.at[idx, me], ss.at[idx], rr.at[idx], device_id=dev(z, q), device_id_type=MESH
        )

    way = 1 + 2 * core
    at_x, at_y = (me // 2 % 2) * 2 + me // 16, me // 4 % 4

    def chip(dx, dy, c):
        x, y = (at_x + way * dx) % 4, (at_y + way * dy) % 4
        return (x % 2) * 16 + y * 4 + (x // 2) * 2 + c

    others = [chip(dx, dy, c) for dx, dy in STEPS for c in range(2)] + [me ^ 1]

    def send(idx):
        got[idx, me] = stage[idx, me]
        for q in others:
            xycopy(idx, q).start()

    def last_own():
        return pltpu.make_async_copy(stage.at[7, me], got_o.at[me], lsem.at[6])

    def send_last():
        last_own().start()
        for q in others:
            pltpu.make_async_remote_copy(
                stage.at[7, q], got_o.at[me], ss.at[7], rr.at[7], device_id=dev(z, q), device_id_type=MESH
            ).start()

    def accumulate(idx):
        with jax.named_scope("waitxy"):
            wait_all(got.at[idx, pl.ds(0, NP - 1)], rr.at[idx])
        add_slots(cbuf[idx], got.at[idx], acc)

    def fold(y):
        y = y + pltpu.roll(y, 7, 0)
        return y + pltpu.roll(y, 6, 0)

    def dcopy(q):
        return pltpu.make_async_remote_copy(
            dsend.at[q], drecv.at[me], ds_, dr, device_id=dev(z, q), device_id_type=MESH
        )

    def targets_out(quads):
        row4, block = iota((8, 128), 0) % 4, iota((8, 128), 1) // CAP
        for pq in quads:
            x = mall[:, pq, :] >> 7
            turned = [pltpu.roll(x, s * CAP, 1) if s else x for s in range(4)]
            for j in range(4):
                y = sum(jnp.where((block == row4) & ((row4 + 4 - j) % 4 == s), turned[s], 0) for s in range(4))
                y = fold(y)
                dsend[pq * 4 + j] = y[0:1] + (y[4:5] << 16)

    def targets_first():
        for n in range(3, NZ):
            mcopy(n).wait_recv()
        targets_out(range(4))

    def targets_rest():
        targets_out(range(4, 8))
        drecv[me] = dsend[me]

        @pl.loop(1, NP)
        def _(j):
            dcopy(me ^ j).start()

    def targets_in():
        many = drecv.at[pl.ds(0, NP - 1)]
        pltpu.make_async_copy(many, many, dr).wait()
        row4, block = iota((8, 128), 0) % 4, iota((8, 128), 1) // CAP
        for v in range(4):
            words = drecv[pl.ds(v * 8, 8)].reshape(8, 128)
            for r in range(2):
                x = (words >> 16) if r else (words & 0xFFFF)
                turned = [pltpu.roll(x, s * CAP, 1) if s else x for s in range(4)]
                for m in range(4):
                    y = sum(jnp.where((block == row4) & ((row4 + 4 - m) % 4 == s), turned[s], 0) for s in range(4))
                    y = fold(y)
                    for h in range(2):
                        cbuf[4 * r + m, 2 * v + h : 2 * v + h + 1, :] = y[4 * h : 4 * h + 1]

    def w3copy(t):
        to = (z + t) % NZ
        return pltpu.make_async_remote_copy(
            part.at[to], w3.at[z], ws.at[1], wr.at[1], device_id=dev(to, me), device_id_type=MESH
        )

    def rows_copy(q):
        mine = w4.at[me // 2, core, z]
        return pltpu.make_async_remote_copy(
            mine, mine, ws.at[2], wr.at[2], device_id=dev(z, q), device_id_type=MESH
        )

    def column_copy(t):
        mine = w4.at[:, core, z]
        return pltpu.make_async_remote_copy(
            mine, mine, ws.at[3], wr.at[3], device_id=dev((z + t) % NZ, me), device_id_type=MESH
        )

    def w4side():
        return pltpu.make_async_remote_copy(
            w4.at[:, core], w4_o.at[:, core], ws.at[4], wr.at[4], device_id=dev(z, me ^ 1), device_id_type=MESH
        )

    def w4own():
        return pltpu.make_async_copy(w4.at[:, core], w4_o.at[:, core], lsem.at[2])

    adder = me < RED

    def weight_add():
        @pl.when(adder)
        def _():
            w2[me] = share[pl.ds(pl.multiple_of(me * 32, 32), 32), :]
            wait_all(w2.at[pl.ds(0, NP - 1)], wr.at[0])
            total = w2[0].astype(F32)
            for i in range(1, NP):
                total = total + w2[i].astype(F32)
            part[...] = total.reshape(NZ, 4, D)
            w3[z] = part[z]

            @pl.loop(1, NZ)
            def _(t):
                w3copy(t).start()

    def weight_column():
        @pl.when(adder)
        def _():
            wait_all(w3.at[pl.ds(0, NZ - 1)], wr.at[1])
            total = w3[0]
            for i in range(1, NZ):
                total = total + w3[i]
            w4[me // 2, core, z] = total.astype(BF16)

            @pl.loop(1, NP // 2)
            def _(j):
                rows_copy(me ^ (2 * j)).start()

    def weight_spread():
        @pl.when(adder)
        def _():
            wait_all(w4.at[pl.ds(0, RED // 2 - 1), 0, 0], wr.at[2])

        @pl.when(me >= RED)
        def _():
            wait_all(w4.at[:, 0, 0], wr.at[2])

        @pl.loop(1, NZ)
        def _(t):
            column_copy(t).start()

    def weight_side():
        wait_all(w4.at[:, 0, pl.ds(0, NZ - 1)], wr.at[3])
        w4side().start()
        w4own().start()

    acc[...] = jnp.zeros_like(acc)

    def pass_on(n, c):
        e, t = (n - 1) % 2, (n + 1) // 2
        with jax.named_scope(f"waitz{c}"):
            zcopy(e, t, c).wait_recv()

        @pl.when((t < 3) | (c < NCH // 2))
        def _():
            zcopy(e, t + 1, c).start()

    @pl.loop(0, 9)
    def _(n):
        @pl.when((n > 0) & (n < 7))
        def _():
            pass_on(n, 2)

            @pl.when((n > 1) & (n < 6))
            def _():
                pass_on(n + 1, 0)

            pass_on(n, 3)

        @pl.when(n == 7)
        def _():
            with jax.named_scope("waitz4"):
                for c in range(NCH // 2):
                    for e in range(2):
                        zcopy(e, 4, c).wait_recv()

        @pl.when(n < 8)
        def _():
            @pl.when((n == 1) | (n == 2))
            def _():
                with jax.named_scope("waitm"):
                    mcopy(n).wait_recv()

            with jax.named_scope("gather"):
                gather(n)

            @pl.when(n < 7)
            def _():
                with jax.named_scope("send"):
                    send(n)

            @pl.when(n == 7)
            def _():
                with jax.named_scope("send"):
                    send_last()


        def once(when, what):
            @pl.when(n == when)
            def _():
                with jax.named_scope(what.__name__):
                    what()

        def add(lo, hi):
            @pl.loop(lo, hi)
            def _(m):
                with jax.named_scope("acc"):
                    accumulate(m)

        @pl.when(n < 2)
        def _():
            pass_on(n + 1, 0)

        @pl.when(n < 6)
        def _():
            pass_on(n + 1, 1)

        once(1, weight_add)
        once(2, targets_first)
        once(3, targets_rest)
        once(4, weight_column)
        once(6, targets_in)
        once(7, weight_spread)
        add(jnp.where(n == 8, 1, 0), jnp.where(n == 8, 7, jnp.where(n == 6, 1, 0)))

    outs = [pltpu.make_async_copy(acc, acc_o, lsem.at[0]), pltpu.make_async_copy(cbuf.at[7], code_o, lsem.at[1])]
    for c in outs:
        c.start()
    with jax.named_scope("weight_side"):
        weight_side()
    for t in range(1, 5):
        for d in range(2):
            for c in range(NCH):
                if t < 4 or c < NCH // 2:
                    zcopy(d, t, c).wait_send()
    wait_all(mall.at[pl.ds(0, NZ - 1)], ms)
    wait_all(dsend.at[pl.ds(0, NP - 1)], ds_)
    wait_all(w4.at[:, 0, pl.ds(0, NZ - 1)], ws.at[3])
    for k in range(8):
        wait_all(stage.at[k, pl.ds(0, NP - 1)], ss.at[k])

    @pl.when(adder)
    def _():
        wait_all(w2.at[pl.ds(0, RED - 1)], ws.at[0])
        wait_all(w3.at[pl.ds(0, NZ - 1)], ws.at[1])
        wait_all(w4.at[pl.ds(0, 5), 0, pl.ds(0, 3)], ws.at[2])

    @pl.when(me >= RED)
    def _():
        wait_all(w2.at[pl.ds(0, RED)], ws.at[0])

    for c in outs:
        c.wait()
    last_own().wait()
    with jax.named_scope("waitside"):
        w4own().wait()
        w4side().wait()
    with jax.named_scope("waitxy"):
        wait_all(got_o.at[pl.ds(0, NP - 1)], rr.at[7])


def on_device(pooled, cotangent, bilinear, bag_ids, bag_lens, row_home):
    any_ = pl.BlockSpec(memory_space=pl.ANY)
    dma = pltpu.SemaphoreType.DMA
    acc, got, code, w4 = pl.pallas_call(
        body,
        out_shape=(
            jax.ShapeDtypeStruct((256, F * D), F32),
            jax.ShapeDtypeStruct((NP, CAP, D), BF16),
            jax.ShapeDtypeStruct((8, 128), I32),
            jax.ShapeDtypeStruct((RED // 2, 2, NZ, 4, D), BF16),
        ),
        in_specs=[any_] * 6,
        out_specs=[any_] * 4,
        scratch_shapes=[
            pltpu.VMEM((ROWS, D), BF16),
            pltpu.VMEM((28, TOK, D), BF16),
            pltpu.VMEM((F - 1, D, D), BF16),
            pltpu.VMEM((F, BAG, TOK), I32),
            pltpu.VMEM((F, TOK), I32),
            pltpu.VMEM((512 * F, 128), I32),
            pltpu.VMEM((F, TOK, D), BF16),
            pltpu.VMEM((F - 1, TOK, D), BF16),
            pltpu.VMEM((F - 1, TOK, D), F32),
            pltpu.VMEM((F - 1, TOK, D), F32),
            pltpu.VMEM(((F - 1) * D, D), BF16),
            pltpu.VMEM((F * BAG, 128), I32),
            pltpu.VMEM((F * BAG, 128), F32),
            pltpu.VMEM((F * BAG, 128), F32),
            pltpu.VMEM((64, 128), I32),
            pltpu.VMEM((NZ, 8, 128), I32),
            pltpu.VMEM((NP, 1, 128), I32),
            pltpu.VMEM((NP, 1, 128), I32),
            pltpu.VMEM((NZ, 8, 128), I32),
            pltpu.VMEM((NZ, ROWS, D), BF16),
            pltpu.VMEM((NZ, NP, CAP, D), BF16),
            pltpu.VMEM((NZ, NP, CAP, D), BF16),
            pltpu.VMEM((256, F * D), F32),
            pltpu.VMEM((NP, 32, D), BF16),
            pltpu.VMEM((NZ, 4, D), F32),
            pltpu.VMEM((RED // 2, 2, NZ, 4, D), BF16),
            pltpu.VMEM((NZ, 4, D), F32),
            dma((7,)),
            dma((2, 4, NCH)),
            dma((2, 4, NCH)),
            dma,
            dma((NZ,)),
            dma,
            dma,
            dma((8,)),
            dma((8,)),
            dma((5,)),
            dma((5,)),
        ],
        compiler_params=pltpu.CompilerParams(
            collective_id=0, has_side_effects=True, vmem_limit_bytes=60 * 2**20
        ),
    )(
        pooled.reshape(ROWS, D),
        cotangent.transpose(1, 0, 2),
        bilinear,
        bag_ids.transpose(1, 2, 0),
        bag_lens.transpose(1, 0),
        row_home.reshape(F, 512, 128).transpose(1, 0, 2).reshape(512 * F, 128),
    )
    wg, table = pl.pallas_call(
        finish,
        out_shape=(
            jax.ShapeDtypeStruct(((F - 1) * D, D), F32),
            jax.ShapeDtypeStruct((256 * F, D), F32),
        ),
        in_specs=[any_] * 4,
        out_specs=[any_] * 2,
        scratch_shapes=[
            pltpu.VMEM((256, F * D), F32),
            pltpu.VMEM((NP, CAP, D), BF16),
            pltpu.VMEM((8, 128), I32),
            pltpu.VMEM(((F - 1) * D // 4, 4, D), BF16),
            pltpu.VMEM(((F - 1) * D, D), F32),
            pltpu.VMEM((256, F * D), F32),
            pltpu.VMEM((256 * F, D), F32),
            dma((6,)),
        ],
        compiler_params=pltpu.CompilerParams(vmem_limit_bytes=60 * 2**20),
    )(acc, got, code, w4.reshape((F - 1) * D // 4, 4, D))
    return wg.reshape(F - 1, D, D), table.reshape(256, F, D)


def solution(mesh):
    placed = (
        P(("gx", "gy"), None, None),
        P(("gx", "gy"), None, None),
        P(),
        P(("gx", "gy"), None, None),
        P(("gx", "gy"), None),
        P(),
    )
    return jax.shard_map(
        on_device,
        mesh=mesh,
        in_specs=placed,
        out_specs=(P(), P(("gx", "gy"), None, None)),
        check_vma=False,
    )
```

```python
import functools

import jax
import jax.numpy as jnp
from jax import lax
from jax.experimental import pallas as pl
from jax.experimental.pallas import tpu as pltpu
from jax.sharding import PartitionSpec as P

MESH = pl.DeviceIdType.MESH
F = 8
BAG = 4
D = 128
TOK = 128
CAP = 32
NZ = 8
NP = 32
ROWS = F * TOK
NCH = 4
RED = 28
PAIR = {(i, j): p for p, (i, j) in enumerate((i, j) for i in range(F) for j in range(i + 1, F))}
STEPS = ((2, 2), (1, 2), (2, 1), (3, 2), (2, 3), (1, 1), (3, 3), (2, 0), (0, 2), (1, 3), (3, 1), (1, 0), (0, 1), (3, 0), (0, 3))
F32, BF16, I32, I16 = jnp.float32, jnp.bfloat16, jnp.int32, jnp.int16


def dev(z, p):
    return (2 * z + p // 16, p % 16)


def iota(shape, dim):
    return lax.broadcasted_iota(I32, shape, dim)


def bf(x):
    return x.astype(F32).astype(BF16)


def onehot(mask):
    return jnp.where(mask, jnp.ones((), BF16), jnp.zeros((), BF16))


def only(mask, x):
    return jnp.where(mask, x, jnp.zeros((), BF16))


def colsum(x):
    acc = x[:16]
    for i in range(16, x.shape[0], 16):
        acc = acc + x[i : i + 16]
    return jnp.sum(acc.astype(F32), axis=0, keepdims=True)


def dot(a, b, ca=1, cb=0):
    return lax.dot_general(a, b, (((ca,), (cb,)), ((), ())), preferred_element_type=F32)


def wait_all(ref, sem):
    pltpu.make_async_copy(ref, ref, sem).wait()


def add_slots(code, rows, acc):
    field, local = (code & 15).astype(F32), bf(code >> 4)
    q_iota = bf(iota((256, 128), 0))
    lhs, rhs = [], []
    for g in range(8):
        fcol = jnp.broadcast_to(field[g : g + 1, :], (128, 128)).T.astype(BF16)
        v = rows[pl.ds(g * 4, 4)].reshape(128, D)
        rhs.append(jnp.concatenate([only(fcol == jnp.asarray(f + 1, BF16), v) for f in range(F)], axis=1))
        lhs.append(onehot(q_iota == local[g : g + 1, :]))
        if g % 4 == 3:
            acc[...] += dot(jnp.concatenate(lhs, axis=1), jnp.concatenate(rhs, axis=0))
            lhs, rhs = [], []


def finish(acc_h, got_h, code_h, w4_h, wg_o, tab_o, acc, got, code, w4, wg, part, table, sem):
    loads = [pltpu.make_async_copy(a, b, sem.at[n]) for n, (a, b) in enumerate([(got_h, got), (code_h, code), (w4_h, w4), (acc_h, acc)])]
    for c in loads:
        c.start()
    part[...] = jnp.zeros_like(part)
    loads[0].wait()
    loads[1].wait()
    add_slots(code[...], got, part)
    loads[2].wait()
    wg[...] = w4[...].astype(F32).reshape((F - 1) * D, D)
    wg_out = pltpu.make_async_copy(wg, wg_o, sem.at[4])
    wg_out.start()
    loads[3].wait()
    for f in range(F):
        cols = slice(f * D, f * D + D)
        table[pl.ds(f, 256, stride=F), :] = acc[:, cols] + part[:, cols]
    table_out = pltpu.make_async_copy(table, tab_o, sem.at[5])
    table_out.start()
    wg_out.wait()
    table_out.wait()


def body(
    pool_h, cot_h, bil_h, ids_h, lens_h, home_h,
    acc_o, got_o, code_o, w4_o,
    pool, cot, bil, ids, lens, home,
    pf, up, proj, back, share,
    own, loc, live, m4, mall, dsend, drecv, cbuf,
    vbuf, stage, got,
    acc, w2, w3, w4, part,
    lsem, zs, zr, ms, mr, ds_, dr, ss, rr, ws, wr,
):
    gx, gy = lax.axis_index("gx"), lax.axis_index("gy")
    z, me = gx // 2, (gx % 2) * 16 + gy
    core = gy % 2

    loads = [
        pltpu.make_async_copy(a, b, lsem.at[n])
        for n, (a, b) in enumerate(
            [(pool_h, pool), (bil_h, bil), (cot_h, cot), (ids_h, ids), (lens_h, lens), (home_h, home)]
        )
    ]
    for c in loads:
        c.start()

    bar = pltpu.get_barrier_semaphore()

    for t in (4, 3, 5, 2, 6, 1, 7):
        pl.semaphore_signal(bar, inc=1, device_id=dev((z + t) % NZ, me), device_id_type=MESH)
    for j in range(NP - 1, 0, -1):
        pl.semaphore_signal(bar, inc=1, device_id=dev(z, me ^ j), device_id_type=MESH)

    with jax.named_scope("perm"):
        loads[0].wait()
        perm = jnp.where(iota((128, 128), 1) == (iota((128, 128), 0) % 16) * F + iota((128, 128), 0) // 16, 1.0, 0.0).astype(BF16)
        x = jnp.concatenate([pool[pl.ds(g * 128, 128), :] for g in range(8)], axis=1)
        y = dot(perm, x).astype(BF16)
        for g in range(8):
            for f in range(F):
                pf[f, pl.ds(g * 16, 16), :] = y[f * 16 : f * 16 + 16, g * 128 : g * 128 + 128]
    with jax.named_scope("grads"):
        loads[1].wait()
        loads[2].wait()
        for i in range(F - 1):
            proj[i] = dot(pf[i], bil[i])
        for r in range(0, TOK, 16):
            rows = pl.ds(r, 16)
            pj = [pf[j, rows, :].astype(F32) for j in range(F)]
            for i in range(F - 1):
                run = cot[PAIR[i, i + 1], rows, :].astype(F32) * pj[i + 1]
                for j in range(i + 2, F):
                    run = run + cot[PAIR[i, j], rows, :].astype(F32) * pj[j]
                up[i, rows, :] = run.astype(BF16)
        for i in range(F - 1):
            back[i] = dot(up[i], bil[i], 1, 1)
        for r in range(0, TOK, 16):
            rows = pl.ds(r, 16)
            for i in range(F):
                run = back[i, rows, :] if i < F - 1 else cot[PAIR[0, i], rows, :].astype(F32) * proj[0, rows, :]
                for k in range(0 if i < F - 1 else 1, i):
                    run = run + cot[PAIR[k, i], rows, :].astype(F32) * proj[k, rows, :]
                vbuf[0, pl.ds(i * TOK + r, 16), :] = run.astype(BF16)
        for i in range(F - 1):
            share[pl.ds(i * D, D), :] = dot(pf[i], up[i], 0, 0).astype(BF16)

    with jax.named_scope("barrier"):
        pl.semaphore_wait(bar, NP - 1 + NZ - 1)

    piece = ROWS // NCH

    def zcopy(e, t, c):
        src = jnp.where(t == 1, 0, 2 * t - 3 + e)
        dst = jnp.where(t == 4, 7, 2 * t - 1 + e)
        at = jnp.where(e == 0, c, NCH - 1 - c)
        rows = pl.ds(pl.multiple_of(at * piece, piece), piece)
        to = (z + jnp.where(e == core, 1, NZ - 1)) % NZ
        return pltpu.make_async_remote_copy(
            vbuf.at[src, rows], vbuf.at[dst, rows], zs.at[e, t - 1, c], zr.at[e, t - 1, c],
            device_id=dev(to, me), device_id_type=MESH,
        )

    def first_hop(e):
        for c in range(NCH):
            zcopy(e, 1, c).start()

    first_hop(0)

    def w2copy(r):
        return pltpu.make_async_remote_copy(
            share.at[pl.ds(pl.multiple_of(r * 32, 32), 32)], w2.at[me], ws.at[0], wr.at[0],
            device_id=dev(z, r), device_id_type=MESH,
        )

    def shares_out():
        for j in range(1, NP):
            r = me ^ j

            @pl.when(r < RED)
            def _():
                w2copy(r).start()

    with jax.named_scope("shares_out"):
        shares_out()

    @pl.when(gx >= 0)
    def _():
        with jax.named_scope("lookup"):
            loads[3].wait()
            loads[4].wait()
            loads[5].wait()
            hi_iota, lo_iota = iota((512, 128), 0).astype(I16), bf(iota((128, 128), 0))
            for f in range(F):
                t = home[pl.ds(f, 512, stride=F), :].T
                table = bf(jnp.concatenate([t >> 8, t & 255], axis=0))
                hi, lo = (ids[f] >> 7).astype(I16), bf(ids[f] & 127)
                oh = jnp.concatenate([onehot(hi_iota == hi[k : k + 1]) for k in range(BAG)], axis=1)
                out = dot(table, oh).astype(BF16)
                for k in range(BAG):
                    mask = lo_iota == lo[k : k + 1]
                    cols = slice(k * 128, k * 128 + 128)
                    row = f * BAG + k
                    own[row : row + 1, :] = colsum(only(mask, out[:128, cols])).astype(I32)
                    loc[row : row + 1, :] = colsum(only(mask, out[128:, cols]))
                    live[row : row + 1, :] = jnp.where(lens[f : f + 1, :] > k, float(f + 1), 0.0)

    first_hop(1)

    @pl.when(gx >= 0)
    def _():
        with jax.named_scope("rank"):
            tri = jnp.where(iota((256, 256), 0) <= iota((256, 256), 1), 1.0, 0.0).astype(BF16)
            own_iota, o4_iota, rr_iota = bf(iota((256, 128), 0)), bf(iota((64, 128), 0)), bf(iota((128, 128), 0))
            lane = bf(iota((1, 128), 1) + 1)
            o = own[...]
            o_b, o4_b, oc_b = bf(o), bf(o >> 2), bf((o & 3) * CAP - 1)
            loc_b, live_b = loc[...].astype(BF16), live[...].astype(BF16)
            before = jnp.zeros((256, 128), BF16)
            lhs, rhs = [], []
            for j in range(16):
                hit = [own_iota == o_b[r : r + 1] for r in (2 * j, 2 * j + 1)]
                count = dot(jnp.concatenate([onehot(h) for h in hit], axis=1), tri).astype(BF16)
                for n in range(2):
                    r = slice(2 * j + n, 2 * j + n + 1)
                    rank = colsum(only(hit[n], count[:, n * 128 : n * 128 + 128] + before))
                    spot = rr_iota == oc_b[r] + rank.astype(BF16)
                    four = o4_iota == o4_b[r]
                    lhs.append(jnp.concatenate([only(spot, lane), only(spot, loc_b[r])], axis=0))
                    rhs.append(jnp.concatenate([onehot(four), only(four, live_b[r])], axis=0))
                before = before + jnp.broadcast_to(count[:, 255:], (256, 128))
            table = dot(jnp.concatenate(lhs, axis=1), jnp.concatenate(rhs, axis=1), 1, 1).T
            b1 = table[:64, :128]
            f1 = jnp.round(table[64:, :128] / jnp.maximum(b1, 1.0))
            m4[...] = jnp.where(b1 > 0, (b1 - 1.0) + 128.0 * f1 + 2048.0 * table[:64, 128:], 0.0).astype(I32)
    mall[0] = m4[pl.ds(pl.multiple_of(z * 8, 8), 8), :]

    def mcopy(n):
        t = (n + 1) // 2
        to = (z + jnp.where((n - 1) % 2 == core, t, NZ - t)) % NZ
        return pltpu.make_async_remote_copy(
            m4.at[pl.ds(pl.multiple_of(to * 8, 8), 8)], mall.at[n], ms, mr.at[n], device_id=dev(to, me), device_id_type=MESH
        )

    @pl.loop(1, NZ)
    def _(t):
        mcopy(t).start()


    lane128 = iota((128, 128), 1).astype(I16)

    def gather(idx):
        for pq in range(8):
            row = mall[idx, pl.ds(pq, 1), :] & 2047
            col = jnp.broadcast_to(row, (128, 128)).T.astype(I16)
            g = jnp.concatenate([onehot(col == lane128 + jnp.asarray(128 * (f + 1), I16)) for f in range(F)], axis=1)
            rows = dot(g, vbuf[idx]).astype(BF16)
            stage[idx, pl.ds(pq * 4, 4)] = rows.reshape(4, CAP, D)

    def xycopy(idx, q):
        return pltpu.make_async_remote_copy(
            stage.at[idx, q], got.at[idx, me], ss.at[idx], rr.at[idx], device_id=dev(z, q), device_id_type=MESH
        )

    way = 1 + 2 * core
    at_x, at_y = (me // 2 % 2) * 2 + me // 16, me // 4 % 4

    def chip(dx, dy, c):
        x, y = (at_x + way * dx) % 4, (at_y + way * dy) % 4
        return (x % 2) * 16 + y * 4 + (x // 2) * 2 + c

    others = [chip(dx, dy, c) for dx, dy in STEPS for c in range(2)] + [me ^ 1]

    def send(idx):
        got[idx, me] = stage[idx, me]
        for q in others:
            xycopy(idx, q).start()

    def last_own():
        return pltpu.make_async_copy(stage.at[7, me], got_o.at[me], lsem.at[6])

    def send_last():
        last_own().start()
        for q in others:
            pltpu.make_async_remote_copy(
                stage.at[7, q], got_o.at[me], ss.at[7], rr.at[7], device_id=dev(z, q), device_id_type=MESH
            ).start()

    def accumulate(idx):
        with jax.named_scope("waitxy"):
            wait_all(got.at[idx, pl.ds(0, NP - 1)], rr.at[idx])
        add_slots(cbuf[idx], got.at[idx], acc)

    def fold(y):
        y = y + pltpu.roll(y, 7, 0)
        return y + pltpu.roll(y, 6, 0)

    def dcopy(q):
        return pltpu.make_async_remote_copy(
            dsend.at[q], drecv.at[me], ds_, dr, device_id=dev(z, q), device_id_type=MESH
        )

    def targets_out(quads):
        row4, block = iota((8, 128), 0) % 4, iota((8, 128), 1) // CAP
        for pq in quads:
            x = mall[:, pq, :] >> 7
            turned = [pltpu.roll(x, s * CAP, 1) if s else x for s in range(4)]
            for j in range(4):
                y = sum(jnp.where((block == row4) & ((row4 + 4 - j) % 4 == s), turned[s], 0) for s in range(4))
                y = fold(y)
                dsend[pq * 4 + j] = y[0:1] + (y[4:5] << 16)

    def targets_first():
        for n in range(3, NZ):
            mcopy(n).wait_recv()
        targets_out(range(4))

    def targets_rest():
        targets_out(range(4, 8))
        drecv[me] = dsend[me]

        for q in others:
            dcopy(q).start()

    def targets_in():
        many = drecv.at[pl.ds(0, NP - 1)]
        pltpu.make_async_copy(many, many, dr).wait()
        row4, block = iota((8, 128), 0) % 4, iota((8, 128), 1) // CAP
        for v in range(4):
            words = drecv[pl.ds(v * 8, 8)].reshape(8, 128)
            for r in range(2):
                x = (words >> 16) if r else (words & 0xFFFF)
                turned = [pltpu.roll(x, s * CAP, 1) if s else x for s in range(4)]
                for m in range(4):
                    y = sum(jnp.where((block == row4) & ((row4 + 4 - m) % 4 == s), turned[s], 0) for s in range(4))
                    y = fold(y)
                    for h in range(2):
                        cbuf[4 * r + m, 2 * v + h : 2 * v + h + 1, :] = y[4 * h : 4 * h + 1]

    def w3copy(t):
        to = (z + t) % NZ
        return pltpu.make_async_remote_copy(
            part.at[to], w3.at[z], ws.at[1], wr.at[1], device_id=dev(to, me), device_id_type=MESH
        )

    def rows_copy(q):
        mine = w4.at[me // 2, core, z]
        return pltpu.make_async_remote_copy(
            mine, mine, ws.at[2], wr.at[2], device_id=dev(z, q), device_id_type=MESH
        )

    def column_copy(t):
        mine = w4.at[:, core, z]
        return pltpu.make_async_remote_copy(
            mine, mine, ws.at[3], wr.at[3], device_id=dev((z + t) % NZ, me), device_id_type=MESH
        )

    def w4side():
        return pltpu.make_async_remote_copy(
            w4.at[:, core], w4_o.at[:, core], ws.at[4], wr.at[4], device_id=dev(z, me ^ 1), device_id_type=MESH
        )

    def w4own():
        return pltpu.make_async_copy(w4.at[:, core], w4_o.at[:, core], lsem.at[2])

    adder = me < RED

    def weight_add():
        @pl.when(adder)
        def _():
            w2[me] = share[pl.ds(pl.multiple_of(me * 32, 32), 32), :]
            wait_all(w2.at[pl.ds(0, NP - 1)], wr.at[0])
            total = w2[0].astype(F32)
            for i in range(1, NP):
                total = total + w2[i].astype(F32)
            part[...] = total.reshape(NZ, 4, D)
            w3[z] = part[z]

            @pl.loop(1, NZ)
            def _(t):
                w3copy(t).start()

    def weight_column():
        @pl.when(adder)
        def _():
            wait_all(w3.at[pl.ds(0, NZ - 1)], wr.at[1])
            total = w3[0]
            for i in range(1, NZ):
                total = total + w3[i]
            w4[me // 2, core, z] = total.astype(BF16)

            @pl.loop(1, NP // 2)
            def _(j):
                rows_copy(me ^ (2 * j)).start()

    def weight_spread():
        @pl.when(adder)
        def _():
            wait_all(w4.at[pl.ds(0, RED // 2 - 1), 0, 0], wr.at[2])

        @pl.when(me >= RED)
        def _():
            wait_all(w4.at[:, 0, 0], wr.at[2])

        @pl.loop(1, NZ)
        def _(t):
            column_copy(t).start()

    def weight_side():
        wait_all(w4.at[:, 0, pl.ds(0, NZ - 1)], wr.at[3])
        w4side().start()
        w4own().start()

    acc[...] = jnp.zeros_like(acc)

    def pass_on(n, c):
        e, t = (n - 1) % 2, (n + 1) // 2
        with jax.named_scope(f"waitz{c}"):
            zcopy(e, t, c).wait_recv()

        @pl.when((t < 3) | (c < NCH // 2))
        def _():
            zcopy(e, t + 1, c).start()

    @pl.loop(0, 9)
    def _(n):
        @pl.when((n > 0) & (n < 7))
        def _():
            pass_on(n, 2)

            @pl.when((n > 1) & (n < 6))
            def _():
                pass_on(n + 1, 0)

            pass_on(n, 3)

        @pl.when(n == 7)
        def _():
            with jax.named_scope("waitz4"):
                for c in range(NCH // 2):
                    for e in range(2):
                        zcopy(e, 4, c).wait_recv()

        @pl.when(n < 8)
        def _():
            @pl.when((n == 1) | (n == 2))
            def _():
                with jax.named_scope("waitm"):
                    mcopy(n).wait_recv()

            with jax.named_scope("gather"):
                gather(n)

            @pl.when(n < 7)
            def _():
                with jax.named_scope("send"):
                    send(n)

            @pl.when(n == 7)
            def _():
                with jax.named_scope("send"):
                    send_last()


        def once(when, what):
            @pl.when(n == when)
            def _():
                with jax.named_scope(what.__name__):
                    what()

        def add(lo, hi):
            @pl.loop(lo, hi)
            def _(m):
                with jax.named_scope("acc"):
                    accumulate(m)

        @pl.when(n < 2)
        def _():
            pass_on(n + 1, 0)

        @pl.when(n < 6)
        def _():
            pass_on(n + 1, 1)

        once(1, weight_add)
        once(2, targets_first)
        once(3, targets_rest)
        once(4, weight_column)
        once(6, targets_in)
        once(7, weight_spread)
        add(jnp.where(n == 8, 1, 0), jnp.where(n == 8, 7, jnp.where(n == 6, 1, 0)))

    outs = [pltpu.make_async_copy(acc, acc_o, lsem.at[0]), pltpu.make_async_copy(cbuf.at[7], code_o, lsem.at[1])]
    for c in outs:
        c.start()
    with jax.named_scope("weight_side"):
        weight_side()
    for t in range(1, 5):
        for d in range(2):
            for c in range(NCH):
                if t < 4 or c < NCH // 2:
                    zcopy(d, t, c).wait_send()
    wait_all(mall.at[pl.ds(0, NZ - 1)], ms)
    wait_all(dsend.at[pl.ds(0, NP - 1)], ds_)
    wait_all(w4.at[:, 0, pl.ds(0, NZ - 1)], ws.at[3])
    for k in range(8):
        wait_all(stage.at[k, pl.ds(0, NP - 1)], ss.at[k])

    @pl.when(adder)
    def _():
        wait_all(w2.at[pl.ds(0, RED - 1)], ws.at[0])
        wait_all(w3.at[pl.ds(0, NZ - 1)], ws.at[1])
        wait_all(w4.at[pl.ds(0, 5), 0, pl.ds(0, 3)], ws.at[2])

    @pl.when(me >= RED)
    def _():
        wait_all(w2.at[pl.ds(0, RED)], ws.at[0])

    for c in outs:
        c.wait()
    last_own().wait()
    with jax.named_scope("waitside"):
        w4own().wait()
        w4side().wait()
    with jax.named_scope("waitxy"):
        wait_all(got_o.at[pl.ds(0, NP - 1)], rr.at[7])


def on_device(pooled, cotangent, bilinear, bag_ids, bag_lens, row_home):
    any_ = pl.BlockSpec(memory_space=pl.ANY)
    dma = pltpu.SemaphoreType.DMA
    acc, got, code, w4 = pl.pallas_call(
        body,
        out_shape=(
            jax.ShapeDtypeStruct((256, F * D), F32),
            jax.ShapeDtypeStruct((NP, CAP, D), BF16),
            jax.ShapeDtypeStruct((8, 128), I32),
            jax.ShapeDtypeStruct((RED // 2, 2, NZ, 4, D), BF16),
        ),
        in_specs=[any_] * 6,
        out_specs=[any_] * 4,
        scratch_shapes=[
            pltpu.VMEM((ROWS, D), BF16),
            pltpu.VMEM((28, TOK, D), BF16),
            pltpu.VMEM((F - 1, D, D), BF16),
            pltpu.VMEM((F, BAG, TOK), I32),
            pltpu.VMEM((F, TOK), I32),
            pltpu.VMEM((512 * F, 128), I32),
            pltpu.VMEM((F, TOK, D), BF16),
            pltpu.VMEM((F - 1, TOK, D), BF16),
            pltpu.VMEM((F - 1, TOK, D), F32),
            pltpu.VMEM((F - 1, TOK, D), F32),
            pltpu.VMEM(((F - 1) * D, D), BF16),
            pltpu.VMEM((F * BAG, 128), I32),
            pltpu.VMEM((F * BAG, 128), F32),
            pltpu.VMEM((F * BAG, 128), F32),
            pltpu.VMEM((64, 128), I32),
            pltpu.VMEM((NZ, 8, 128), I32),
            pltpu.VMEM((NP, 1, 128), I32),
            pltpu.VMEM((NP, 1, 128), I32),
            pltpu.VMEM((NZ, 8, 128), I32),
            pltpu.VMEM((NZ, ROWS, D), BF16),
            pltpu.VMEM((NZ, NP, CAP, D), BF16),
            pltpu.VMEM((NZ, NP, CAP, D), BF16),
            pltpu.VMEM((256, F * D), F32),
            pltpu.VMEM((NP, 32, D), BF16),
            pltpu.VMEM((NZ, 4, D), F32),
            pltpu.VMEM((RED // 2, 2, NZ, 4, D), BF16),
            pltpu.VMEM((NZ, 4, D), F32),
            dma((7,)),
            dma((2, 4, NCH)),
            dma((2, 4, NCH)),
            dma,
            dma((NZ,)),
            dma,
            dma,
            dma((8,)),
            dma((8,)),
            dma((5,)),
            dma((5,)),
        ],
        compiler_params=pltpu.CompilerParams(
            collective_id=0, has_side_effects=True, vmem_limit_bytes=60 * 2**20
        ),
    )(
        pooled.reshape(ROWS, D),
        cotangent.transpose(1, 0, 2),
        bilinear,
        bag_ids.transpose(1, 2, 0),
        bag_lens.transpose(1, 0),
        row_home.reshape(F, 512, 128).transpose(1, 0, 2).reshape(512 * F, 128),
    )
    wg, table = pl.pallas_call(
        finish,
        out_shape=(
            jax.ShapeDtypeStruct(((F - 1) * D, D), F32),
            jax.ShapeDtypeStruct((256 * F, D), F32),
        ),
        in_specs=[any_] * 4,
        out_specs=[any_] * 2,
        scratch_shapes=[
            pltpu.VMEM((256, F * D), F32),
            pltpu.VMEM((NP, CAP, D), BF16),
            pltpu.VMEM((8, 128), I32),
            pltpu.VMEM(((F - 1) * D // 4, 4, D), BF16),
            pltpu.VMEM(((F - 1) * D, D), F32),
            pltpu.VMEM((256, F * D), F32),
            pltpu.VMEM((256 * F, D), F32),
            dma((6,)),
        ],
        compiler_params=pltpu.CompilerParams(vmem_limit_bytes=60 * 2**20),
    )(acc, got, code, w4.reshape((F - 1) * D // 4, 4, D))
    return wg.reshape(F - 1, D, D), table.reshape(256, F, D)


def solution(mesh):
    placed = (
        P(("gx", "gy"), None, None),
        P(("gx", "gy"), None, None),
        P(),
        P(("gx", "gy"), None, None),
        P(("gx", "gy"), None),
        P(),
    )
    return jax.shard_map(
        on_device,
        mesh=mesh,
        in_specs=placed,
        out_specs=(P(), P(("gx", "gy"), None, None)),
        check_vma=False,
    )
```
